32 devices in a mesh: dp: 4 (over x, core), expert: 8 (over z, y).
Axes of the slice: x: 2, y: 2, z: 4, core: 2. Of those that a mesh axis runs over, the one named last changes fastest.
Arguments:
- tokens: bfloat16 [32768, 512], P(('dp', 'expert')), may hold values from -6 to 6
- cotangent: bfloat16 [32768, 512], P(('dp', 'expert')), may hold values from -6 to 6
- valid: int32 [128, 256], P(('dp', 'expert')), may hold values from 0 to 1, as said below
- routes: int32 [2, 32768, 2], P(None, ('dp', 'expert')), may hold values from 0 to 7, all different within a row
- priority: int32 [64, 512], P(('dp', 'expert')), may hold values from 0 to 511, each once within a row
- step: int32 [], replicated, may hold values from 1 to 20
- dense_master: float32 [2, 2064, 512], P(None, 'dp'), may hold values from -2 to 2
- dense_first: float32 [2, 2064, 512], P(None, 'dp'), may hold values from -0.00024414062 to 0.00024414062
- dense_second: float32 [2, 2064, 512], P(None, 'dp'), may hold values from 1.4194222e-09 to 1.4194222e-07
- expert_master: float32 [2, 8, 1024, 2048], P(None, 'expert', 'dp'), may hold values from -0.494974747 to 0.494974747
- expert_first: float32 [2, 8, 1024, 2048], P(None, 'expert', 'dp'), may hold values from -0.00024414062 to 0.00024414062
- expert_second: float32 [2, 8, 1024, 2048], P(None, 'expert', 'dp'), may hold values from 2.8004202e-10 to 8.40126e-09
- shift_master: float32 [2, 8, 2560], P(None, 'expert', 'dp'), may hold values from -5.6 to 5.6
- shift_first: float32 [2, 8, 2560], P(None, 'expert', 'dp'), may hold values from -0.00024414062 to 0.00024414062
- shift_second: float32 [2, 8, 2560], P(None, 'expert', 'dp'), may hold values from 2.8004202e-10 to 8.40126e-09
Outputs:
- output: float32 [32768, 512], P(('dp', 'expert'))
- grad_tokens: float32 [32768, 512], P(('dp', 'expert'))
- grad_norm: float32 [], replicated
- dense_grad: float32 [2, 2064, 512], P(None, 'dp')
- dense_update: float32 [2, 2064, 512], P(None, 'dp')
- dense_first_new: float32 [2, 2064, 512], P(None, 'dp')
- dense_second_new: float32 [2, 2064, 512], P(None, 'dp')
- expert_grad: float32 [2, 8, 1024, 2048], P(None, 'expert', 'dp')
- expert_update: float32 [2, 8, 1024, 2048], P(None, 'expert', 'dp')
- expert_first_new: float32 [2, 8, 1024, 2048], P(None, 'expert', 'dp')
- expert_second_new: float32 [2, 8, 1024, 2048], P(None, 'expert', 'dp')
- shift_grad: float32 [2, 8, 2560], P(None, 'expert', 'dp')
- shift_update: float32 [2, 8, 2560], P(None, 'expert', 'dp')
- shift_first_new: float32 [2, 8, 2560], P(None, 'expert', 'dp')
- shift_second_new: float32 [2, 8, 2560], P(None, 'expert', 'dp')
The draws below stay inside these ranges and needn't reach their ends.
Inputs may be any that keep to these rules, and one draw needn't show every extreme that they name: `valid`: each image's row is 0 everywhere, or 1 exactly in its first 197 slots. `routes`: each token names two different experts. `priority`: each row holds every rank of 0 to 511 once.
All inputs are finite; a program needn't handle non-finite values.
Results may differ from the reference program's by a relative error of at most 0.022.
Values may be sent and summed in bfloat16 or wider, within the bound.
A program may use at most 320 MiB of HBM per device.

```python
import math
import jax
import jax.numpy as jnp
from jax import lax

D = 512
FF = 2048
HEADS = 8
HEAD = 64
PATCHES = 197
SEQ = 256
LAYERS = 2
IMG_MB = 2
GROUP_TOK = 512
EXPERTS = 8
IMAGES = 128
TOKENS = 32768
GROUPS = 64
CAP = 111
DROWS = 2064
PARAMS = 35708928


def draw_valid(key, part):
    real_image = jax.random.randint(key, (IMAGES,), 0, 8) < 7
    in_image = jnp.arange(SEQ) < PATCHES
    return (real_image[:, None] & in_image[None, :]).astype(jnp.int32)


def draw_dense_master(key, part):
    noise_vals = jnp.clip(jax.random.normal(key, (LAYERS, DROWS, D), jnp.float32), -3.5, 3.5)
    row_ids = jnp.arange(DROWS)
    base_row = 4 * D + EXPERTS
    spread = jnp.where(row_ids < 3 * D, D ** (-0.5), 0.3)
    spread = jnp.where((row_ids >= 3 * D) & (row_ids < 4 * D), 0.7 * (PATCHES / D) ** 0.5, spread)
    spread = jnp.where((row_ids >= 4 * D) & (row_ids < base_row), 1.5 * D ** (-0.5), spread)
    is_gain = (row_ids == base_row) | (row_ids == base_row + 6)
    spread = jnp.where(is_gain, 0.2, spread)
    centre = jnp.where(is_gain, 1.0, 0.0)
    return (centre[None, :, None] + spread[None, :, None] * noise_vals).astype(jnp.float32)


def draw_expert_master(key, part):
    noise_vals = jnp.clip(jax.random.normal(key, (LAYERS, EXPERTS, 2 * D, FF), jnp.float32), -3.5, 3.5)
    row_ids = jnp.arange(2 * D)
    spread = jnp.where(row_ids < D, D ** (-0.5), 0.8 * EXPERTS * FF ** (-0.5))
    return (spread[None, None, :, None] * noise_vals).astype(jnp.float32)


def draw_shift_master(key, part):
    noise_vals = jnp.clip(jax.random.normal(key, (LAYERS, EXPERTS, FF + D), jnp.float32), -3.5, 3.5)
    col_ids = jnp.arange(FF + D)
    spread = jnp.where(col_ids < FF, 0.5, 0.2 * EXPERTS)
    return (spread[None, None, :] * noise_vals).astype(jnp.float32)


def steps_of(own_key, extent, shards, least, top_value):
    def one(axis_at, shards_of):
        draws = jax.random.uniform(jax.random.fold_in(jax.random.fold_in(own_key, 6), axis_at), (shards_of,), jnp.float32, least / len(shards), top_value / len(shards))
        return jnp.repeat(jnp.exp(draws), extent[axis_at] // shards_of).reshape((-1,) + (1,) * (len(extent) - axis_at - 1))

    loudness = one(*shards[0])
    for cut in shards[1:]:
        loudness = loudness * one(*cut)
    return loudness


def distinct(rng, rows, count, top, lift):
    sequence = jax.random.permutation(jax.random.fold_in(rng, 1), count)
    boost = sequence
    for power in range(3):
        boost = boost * boost // count
    boost = boost * lift // count
    tickets = jax.random.randint(jax.random.fold_in(rng, 2), (rows, count), 0, 4096) + boost
    sure = jax.random.permutation(jax.random.fold_in(rng, 3), rows)[jnp.arange(count) % rows]
    tickets = jnp.where(jnp.arange(rows)[:, None] == sure[None, :], 1 << 14, tickets)
    merit = tickets * count + jnp.arange(count)
    return lax.top_k(merit.astype(jnp.int32), top)[1].astype(jnp.int32)


def noise(stream_key, shape, scale, most, split=(), kind=jnp.bfloat16):
    drawn = scale * jax.random.normal(stream_key, shape, jnp.float32)
    if split:
        drawn = drawn * steps_of(stream_key, shape, split, -0.22, 0.18)
    return jnp.clip(drawn, -most, most).astype(kind)


def setup_inputs(seed: int = 0) -> dict:
    key_of = jax.random.split(jax.random.key(seed), 16)
    tokens = noise(key_of[0], (TOKENS, D), 1.0, 6.0, ((0, 32),))
    cotangent = noise(key_of[1], (TOKENS, D), 1.0, 6.0, ((0, 32),))
    valid = draw_valid(jax.random.fold_in(key_of[15], 71), 0)
    routes = distinct(key_of[3], LAYERS * TOKENS, EXPERTS, 2, 2048).reshape((LAYERS, TOKENS, 2))
    priority = jax.vmap(lambda own: jax.random.permutation(own, GROUP_TOK))(jax.random.split(key_of[4], GROUPS)).reshape((GROUPS, GROUP_TOK)).astype(jnp.int32)
    step = jax.random.randint(key_of[5], (), 1, 21).astype(jnp.int32)
    dense_master = draw_dense_master(jax.random.fold_in(key_of[15], 71), 0)
    dense_first = noise(key_of[7], (LAYERS, DROWS, D), (0.11 * PARAMS ** -0.5), 0.00024414062, ((1, 4),), jnp.float32)
    dense_second = jnp.clip(jnp.exp(math.log(1.419422233084333e-07) - 4.6051702 * jax.random.uniform(key_of[8], (LAYERS, DROWS, D), jnp.float32) ** steps_of(key_of[8], (LAYERS, DROWS, D), ((1, 4),), -0.2, 0.2)), 1.4194222464070094e-09, 1.419422233084333e-07)
    expert_master = draw_expert_master(jax.random.fold_in(key_of[15], 71), 0)
    expert_first = noise(key_of[10], (LAYERS, EXPERTS, 2 * D, FF), (0.11 * PARAMS ** -0.5), 0.00024414062, ((1, 8), (2, 4)), jnp.float32)
    expert_second = jnp.clip(jnp.exp(math.log(8.401260132018251e-09) - 3.40119734 * jax.random.uniform(key_of[11], (LAYERS, EXPERTS, 2 * D, FF), jnp.float32) ** steps_of(key_of[11], (LAYERS, EXPERTS, 2 * D, FF), ((1, 8), (2, 4)), -0.2, 0.2)), 2.8004201735321033e-10, 8.401260132018251e-09)
    shift_master = draw_shift_master(jax.random.fold_in(key_of[15], 71), 0)
    shift_first = noise(key_of[13], (LAYERS, EXPERTS, FF + D), (0.11 * PARAMS ** -0.5), 0.00024414062, ((1, 8), (2, 4)), jnp.float32)
    shift_second = jnp.clip(jnp.exp(math.log(8.401260132018251e-09) - 3.40119734 * jax.random.uniform(key_of[14], (LAYERS, EXPERTS, FF + D), jnp.float32) ** steps_of(key_of[14], (LAYERS, EXPERTS, FF + D), ((1, 8), (2, 4)), -0.2, 0.2)), 2.8004201735321033e-10, 8.401260132018251e-09)
    return {"tokens": tokens, "cotangent": cotangent, "valid": valid, "routes": routes, "priority": priority, "step": step, "dense_master": dense_master, "dense_first": dense_first, "dense_second": dense_second, "expert_master": expert_master, "expert_first": expert_first, "expert_second": expert_second, "shift_master": shift_master, "shift_first": shift_first, "shift_second": shift_second}


@jax.custom_vjp
def low(v):
    return lax.optimization_barrier(v.astype(jnp.bfloat16)).astype(jnp.float32)

@jax.custom_vjp
def low_back(v):
    return v

def low_keep(v):
    return (low(v), None)

def low_pass(kept, grad):
    return (grad,)

def back_keep(v):
    return (v, None)

def back_low(kept, grad):
    return (low(grad),)
low.defvjp(low_keep, low_pass)
low_back.defvjp(back_keep, back_low)
NORM_EPS = 1e-06
NEG_FILL = -1e+30
CLIP_NORM = 1.0
BETA_ONE = 0.9
BETA_TWO = 0.95
STEP_RATE = 0.01
DECAY_RATE = 0.1
ADAM_EPS = 1e-08
HIGHEST = lax.Precision.HIGHEST

def norm_rows(values, gain_row, shift_row):
    centred = values - lax.optimization_barrier(jnp.mean(values, axis=-1, keepdims=True))
    spread = lax.optimization_barrier(jnp.mean(centred * centred, axis=-1, keepdims=True))
    return centred * lax.rsqrt(spread + NORM_EPS) * gain_row + shift_row

def erf_gelu(values):
    return jax.nn.gelu(values, approximate=False)

def rounded(values):
    return lax.optimization_barrier(values.astype(jnp.bfloat16)).astype(jnp.float32)

def placement(routed, ranking, usable, experts, capacity):
    tok_count = routed.shape[0]
    positions = jnp.arange(tok_count, dtype=jnp.int32)
    ordering = jnp.zeros((tok_count,), jnp.int32).at[ranking].set(positions)
    labels = jnp.arange(experts, dtype=jnp.int32)
    one_hot = (routed[ordering][:, :, None] == labels).astype(jnp.int32) * usable[ordering][:, None, None]
    earlier = jnp.cumsum(one_hot, axis=0) - one_hot
    first_total = lax.optimization_barrier(jnp.sum(one_hot[:, 0], axis=0))
    pos_first = lax.optimization_barrier(jnp.sum(earlier[:, 0] * one_hot[:, 0], axis=-1))
    pos_second = lax.optimization_barrier(jnp.sum((earlier[:, 1] + first_total[None, :]) * one_hot[:, 1], axis=-1))
    ranked = jnp.stack([pos_first, pos_second], axis=-1)
    position = ranked[ranking]
    keeping = (position < capacity) & (usable[:, None] > 0)
    slot_index = jnp.where(keeping, routed * capacity + position, experts * capacity).astype(jnp.int32)
    slot_source = jnp.full((experts * capacity + 1,), tok_count, jnp.int32)
    slot_source = slot_source.at[slot_index[:, 0]].set(positions).at[slot_index[:, 1]].set(positions)
    return (slot_index, keeping.astype(jnp.float32), slot_source)

def run_block(current, tok_ok, routed, ranking, row_block, mat_block, shift_block):
    tok_count = current.shape[0]
    qkv_rows = row_block[:3 * D]
    out_rows = row_block[3 * D:4 * D]
    router_rows = row_block[4 * D:4 * D + EXPERTS]
    vectors = row_block[4 * D + EXPERTS:]
    normed_a = low(norm_rows(current, vectors[0], vectors[1]))
    qkv_full = low(low_back(jnp.dot(normed_a, qkv_rows.T, precision=HIGHEST) + vectors[2:5].reshape(-1)))
    qkv_parts = qkv_full.reshape(IMG_MB, SEQ, 3, HEADS, HEAD)
    queries = qkv_parts[:, :, 0]
    keys_all = qkv_parts[:, :, 1]
    values_all = qkv_parts[:, :, 2]
    key_ok = tok_ok.reshape(IMG_MB, SEQ) > 0
    scores = low_back(jnp.einsum('bqhd,bkhd->bhqk', queries, keys_all, precision=HIGHEST) * HEAD ** (-0.5))
    scores = jnp.where(key_ok[:, None, None, :], scores, NEG_FILL)
    weights = jax.nn.softmax(scores, axis=-1)
    attended = jnp.einsum('bhqk,bkhd->bqhd', low(weights), values_all, precision=HIGHEST).reshape(tok_count, D)
    attended = low(low_back(attended))
    x_mid = current + low_back(jnp.dot(attended, out_rows, precision=HIGHEST) + vectors[5])
    normed_c = low(norm_rows(x_mid, vectors[6], vectors[7]))
    logits = low_back(jnp.dot(normed_c, router_rows.T, precision=HIGHEST))
    router = jax.nn.softmax(logits, axis=-1)
    choose = (routed[:, :, None] == jnp.arange(EXPERTS, dtype=jnp.int32)).astype(jnp.float32)
    gate_values = lax.optimization_barrier(jnp.sum(router[:, None, :] * choose, axis=-1))
    slot_index, keeping, slot_source = placement(routed, ranking, tok_ok, EXPERTS, CAP)
    padded = jnp.concatenate([normed_c, jnp.zeros((1, D), jnp.float32)], axis=0)
    buffer = low_back(padded[slot_source[:EXPERTS * CAP]].reshape(EXPERTS, CAP, D))
    hidden_pre = low_back(jnp.einsum('ecd,edf->ecf', buffer, mat_block[:, :D], precision=HIGHEST) + shift_block[:, None, :FF])
    active = low(erf_gelu(hidden_pre))
    produced = low(low_back(jnp.einsum('ecf,edf->ecd', active, mat_block[:, D:], precision=HIGHEST) + shift_block[:, None, FF:]))
    flat_rows = jnp.concatenate([produced.reshape(EXPERTS * CAP, D), jnp.zeros((1, D), jnp.float32)], axis=0)
    mixing = keeping * gate_values
    return x_mid + lax.optimization_barrier(jnp.sum(mixing[:, :, None] * flat_rows[slot_index], axis=1))

def adam_update(master, first_mom, second_mom, gradient, clip_scale, step_float):
    clipped = gradient * clip_scale
    first_new = BETA_ONE * first_mom + (1.0 - BETA_ONE) * clipped
    second_new = BETA_TWO * second_mom + (1.0 - BETA_TWO) * clipped * clipped
    first_hat = first_new / (1.0 - BETA_ONE ** step_float)
    second_hat = second_new / (1.0 - BETA_TWO ** step_float)
    change = -STEP_RATE * (first_hat / (jnp.sqrt(second_hat) + ADAM_EPS) + DECAY_RATE * master)
    return (change, first_new, second_new)

def reference(tokens, cotangent, valid, routes, priority, step, dense_master, dense_first, dense_second, expert_master, expert_first, expert_second, shift_master, shift_first, shift_second):
    dense_low = rounded(dense_master)
    mats_low = rounded(expert_master)
    shift_low = rounded(shift_master)
    token_groups = tokens.astype(jnp.float32).reshape(GROUPS, GROUP_TOK, D)
    seed_groups = cotangent.astype(jnp.float32).reshape(GROUPS, GROUP_TOK, D)
    valid_groups = valid.reshape(GROUPS, GROUP_TOK)
    route_groups = jnp.transpose(routes.reshape(LAYERS, GROUPS, GROUP_TOK, 2), (1, 0, 2, 3))

    def group_step(carry, pieces):
        current, grad_seed, tok_ok, routed, ranking = pieces

        def forward(x_in, dense_in, mats_in, shift_in):
            moving = x_in
            for layer_id in range(LAYERS):
                moving = run_block(moving, tok_ok, routed[layer_id], ranking, dense_in[layer_id], mats_in[layer_id], shift_in[layer_id])
            return jnp.where(tok_ok[:, None] > 0, moving, 0.0)
        finals, pullback = jax.vjp(forward, current, dense_low, mats_low, shift_low)
        grad_x, grad_dense, grad_mats, grad_shift = pullback(grad_seed)
        summed = (carry[0] + grad_dense, carry[1] + grad_mats, carry[2] + grad_shift)
        return (summed, (finals, grad_x))
    start = (jnp.zeros_like(dense_low), jnp.zeros_like(mats_low), jnp.zeros_like(shift_low))
    sums, stacked = lax.scan(group_step, start, (token_groups, seed_groups, valid_groups, route_groups, priority))
    dense_grad, expert_grad, shift_grad = sums
    finals, grad_x = stacked
    total = jnp.sum(dense_grad * dense_grad) + jnp.sum(expert_grad * expert_grad) + jnp.sum(shift_grad * shift_grad)
    grad_norm = jnp.sqrt(total)
    clip_scale = CLIP_NORM / jnp.maximum(grad_norm, CLIP_NORM)
    step_float = step.astype(jnp.float32)
    dense_new = adam_update(dense_master, dense_first, dense_second, dense_grad, clip_scale, step_float)
    expert_new = adam_update(expert_master, expert_first, expert_second, expert_grad, clip_scale, step_float)
    shift_new = adam_update(shift_master, shift_first, shift_second, shift_grad, clip_scale, step_float)
    return (finals.reshape(TOKENS, D), grad_x.reshape(TOKENS, D), grad_norm, dense_grad, dense_new[0], dense_new[1], dense_new[2], expert_grad, expert_new[0], expert_new[1], expert_new[2], shift_grad, shift_new[0], shift_new[1], shift_new[2])
```

```python
import functools

import jax
import jax.numpy as jnp
from jax import lax
from jax.experimental import pallas as pl
from jax.experimental.pallas import tpu as pltpu
from jax.sharding import PartitionSpec as P

HEADS = 8
PATCHES = 197


NORM_EPS = 1e-06
NEG_FILL = -1e30
CLIP_NORM = 1.0
BETA_ONE = 0.9
BETA_TWO = 0.95
STEP_RATE = 0.01
DECAY_RATE = 0.1
ADAM_EPS = 1e-08
LANES = 128
MESH = pl.DeviceIdType.MESH
VMEM_LIMIT = 60 * 1024 * 1024
F32 = jnp.float32
BF16 = jnp.bfloat16
INV_SQRT2 = 0.7071067811865476
INV_SQRT2PI = 0.3989422804014327


def up_to(count, step):
    return -(-count // step) * step


def dot_nn(left, right):
    return lax.dot_general(left, right, (((1,), (0,)), ((), ())), preferred_element_type=F32)


def dot_nt(left, right):
    return lax.dot_general(left, right, (((1,), (1,)), ((), ())), preferred_element_type=F32)


def dot_tn(left, right):
    return lax.dot_general(left, right, (((0,), (0,)), ((), ())), preferred_element_type=F32)


def lane_ids(rows, cols=LANES):
    return lax.broadcasted_iota(jnp.int32, (rows, cols), 1)


def one_where(mask):
    return jnp.where(mask, 1.0, 0.0).astype(BF16)


def normalise(values):
    centred = values - jnp.mean(values, axis=-1, keepdims=True)
    spread = jnp.mean(centred * centred, axis=-1, keepdims=True)
    scale = lax.rsqrt(spread + NORM_EPS)
    return centred * scale, scale


def norm_back(grad_hat, hat, scale):
    return scale * (
        grad_hat
        - jnp.mean(grad_hat, axis=-1, keepdims=True)
        - hat * jnp.mean(grad_hat * hat, axis=-1, keepdims=True)
    )


def dense_parts(dense_ref, experts):
    width = dense_ref.shape[-1]
    tail = dense_ref[4 * width :, :].astype(F32)
    vectors = tail[experts : experts + 8]
    router_rows = jnp.concatenate(
        [tail[:experts], jnp.zeros((LANES - experts, width), F32)], axis=0
    ).astype(BF16)
    return router_rows, vectors


def routing_kernel(capacity, slots_each, experts, layers, meta_ref, cols_ref, slot_col_ref, slot_row_ref):
    toks = meta_ref.shape[-1]
    meta = meta_ref[...]
    cols = cols_ref[...]
    rank_row, rank_col = meta[0:1], cols[:, 0:1]
    ok_row, ok_col = meta[1:2], cols[:, 1:2]
    before = one_where(rank_row < rank_col)
    before_t = one_where(rank_col < rank_row)
    lanes = lane_ids(toks)
    subs = lax.broadcasted_iota(jnp.int32, (LANES, toks), 0)
    col_out = [None] * 16
    row_out = [None] * 8
    for layer in range(layers):
        counts, ones, counts_t, ones_t, totals, totals_t = [], [], [], [], [], []
        for k in range(2):
            named = cols[:, 2 + 2 * layer + k : 3 + 2 * layer + k]
            hot = jnp.where((lanes == named) & (ok_col > 0), 1.0, 0.0)
            ones.append(hot)
            counts.append(dot_nn(before, hot.astype(BF16)))
            totals.append(jnp.sum(hot, axis=0, keepdims=True))
            named_t = meta[2 + 2 * layer + k : 3 + 2 * layer + k]
            hot_t = jnp.where((subs == named_t) & (ok_row > 0), 1.0, 0.0)
            ones_t.append(hot_t)
            counts_t.append(dot_nn(hot_t.astype(BF16), before_t))
            totals_t.append(jnp.sum(hot_t, axis=1, keepdims=True))
        for k in range(2):
            extra = totals[0] if k else 0.0
            place = jnp.sum((counts[k] + extra) * ones[k], axis=1, keepdims=True).astype(jnp.int32)
            named = cols[:, 2 + 2 * layer + k : 3 + 2 * layer + k]
            held = (place < capacity) & (ok_col > 0)
            col_out[2 * layer + k] = jnp.where(held, named * slots_each + place, -1)
            col_out[4 + 2 * layer + k] = named
            extra_t = totals_t[0] if k else 0.0
            place_t = jnp.sum((counts_t[k] + extra_t) * ones_t[k], axis=0, keepdims=True).astype(jnp.int32)
            named_t = meta[2 + 2 * layer + k : 3 + 2 * layer + k]
            held_t = (place_t < capacity) & (ok_row > 0)
            row_out[2 * layer + k] = jnp.where(held_t, named_t * slots_each + place_t, -1)
    col_out[8] = ok_col
    full = jnp.zeros((toks, LANES), jnp.int32)
    for at, value in enumerate(col_out):
        if value is not None:
            full = jnp.where(lanes == at, value, full)
    slot_col_ref[...] = full
    eight = lax.broadcasted_iota(jnp.int32, (8, toks), 0)
    rows = jnp.zeros((8, toks), jnp.int32)
    for at, value in enumerate(row_out):
        if value is not None:
            rows = jnp.where(eight == at, value, rows)
    slot_row_ref[...] = rows


def routing(meta, cols, capacity, slots_each, experts, layers):
    micros, _, toks = meta.shape
    return pl.pallas_call(
        functools.partial(routing_kernel, capacity, slots_each, experts, layers),
        grid=(micros,),
        in_specs=[
            pl.BlockSpec((None, 8, toks), lambda m: (m, 0, 0)),
            pl.BlockSpec((None, toks, 8), lambda m: (m, 0, 0)),
        ],
        out_specs=[
            pl.BlockSpec((None, toks, LANES), lambda m: (m, 0, 0)),
            pl.BlockSpec((None, 8, toks), lambda m: (m, 0, 0)),
        ],
        out_shape=[
            jax.ShapeDtypeStruct((micros, toks, LANES), jnp.int32),
            jax.ShapeDtypeStruct((micros, 8, toks), jnp.int32),
        ],
        compiler_params=pltpu.CompilerParams(vmem_limit_bytes=VMEM_LIMIT),
        name="routing",
    )(meta, cols)


def gates(router, slot_col, layer):
    lanes = lane_ids(router.shape[0])
    out = []
    for k in range(2):
        named = slot_col[:, 4 + 2 * layer + k : 5 + 2 * layer + k]
        value = jnp.sum(jnp.where(lanes == named, router, 0.0), axis=1, keepdims=True)
        held = slot_col[:, 2 * layer + k : 2 * layer + k + 1] >= 0
        out.append(jnp.where(held, value, 0.0))
    return out


def pick_mask(slot_col, layer, k, slots):
    toks = slot_col.shape[0]
    return lax.broadcasted_iota(jnp.int32, (toks, slots), 1) == slot_col[:, 2 * layer + k : 2 * layer + k + 1]


def place_mask(slot_row, layer, k, slots):
    toks = slot_row.shape[1]
    return lax.broadcasted_iota(jnp.int32, (slots, toks), 0) == slot_row[2 * layer + k : 2 * layer + k + 1]


def half_mask(rows, half):
    lanes = lane_ids(rows)
    return (lanes >= LANES // 2) if half else (lanes < LANES // 2)


def attention_forward(x, layer, images, experts, dense_ref, slot_col, slot_row, qkv_ref, a_ref, o_ref, x1_ref, c_ref, router_ref, send_ref):
    toks, width = x.shape
    rows = toks // images
    router_rows, vec = dense_parts(dense_ref, experts)
    hat, _ = normalise(x)
    a = (hat * vec[0:1] + vec[1:2]).astype(BF16)
    a_ref[...] = a
    for part in range(3):
        at = slice(part * width, (part + 1) * width)
        qkv_ref[:, at] = (dot_nt(a, dense_ref[at, :]) + vec[2 + part : 3 + part]).astype(BF16)
    key_dead = lane_ids(rows, rows) >= PATCHES
    scale = (width // HEADS) ** (-0.5)
    for image in range(images):
        at = slice(image * rows, (image + 1) * rows)
        for pair in range(width // LANES):
            q2 = qkv_ref[at, pair * LANES : (pair + 1) * LANES]
            k2 = qkv_ref[at, width + pair * LANES : width + (pair + 1) * LANES]
            v2 = qkv_ref[at, 2 * width + pair * LANES : 2 * width + (pair + 1) * LANES]
            both = []
            for half in range(2):
                q_half = jnp.where(half_mask(rows, half), q2, jnp.zeros_like(q2))
                s = jnp.where(key_dead, NEG_FILL, dot_nt(q_half, k2) * scale)
                e = jnp.exp(s - jnp.max(s, axis=1, keepdims=True))
                p = e * (1.0 / jnp.sum(e, axis=1, keepdims=True))
                both.append(dot_nn(p.astype(BF16), v2))
            o2 = jnp.where(half_mask(rows, 0), both[0], both[1])
            o_ref[at, pair * LANES : (pair + 1) * LANES] = o2.astype(BF16)
    x1 = x + (dot_nn(o_ref[...], dense_ref[3 * width : 4 * width, :]) + vec[5:6])
    x1_ref[...] = x1
    hat, _ = normalise(x1)
    c = (hat * vec[6:7] + vec[7:8]).astype(BF16)
    c_ref[...] = c
    logits = jnp.where(lane_ids(toks) < experts, dot_nt(c, router_rows), NEG_FILL)
    e = jnp.exp(logits - jnp.max(logits, axis=1, keepdims=True))
    router_ref[...] = e / jnp.sum(e, axis=1, keepdims=True)
    slots = send_ref.shape[0] * send_ref.shape[1]
    place = one_where(place_mask(slot_row, layer, 0, slots) | place_mask(slot_row, layer, 1, slots))
    send_ref[...] = dot_nn(place, c).astype(BF16).reshape(send_ref.shape)


def combine(x1, router, slot_col, layer, back, picked_ref):
    slots = back.shape[0] * back.shape[1]
    y = back.reshape(slots, back.shape[2])
    g = gates(router, slot_col, layer)
    total = x1
    for k in range(2):
        picked = dot_nn(one_where(pick_mask(slot_col, layer, k, slots)), y)
        picked_ref[k] = picked.astype(BF16)
        total = total + g[k] * picked
    return total


def combine_back(dx2, router, slot_col, slot_row, layer, picked_ref, dg_ref, send_ref):
    slots = send_ref.shape[0] * send_ref.shape[1]
    toks = dx2.shape[0]
    g = gates(router, slot_col, layer)
    lanes = lane_ids(toks)
    out = jnp.zeros((toks, LANES), F32)
    total = None
    for k in range(2):
        held = slot_col[:, 2 * layer + k : 2 * layer + k + 1] >= 0
        dg = jnp.sum(dx2 * picked_ref[k].astype(F32), axis=1, keepdims=True)
        named = slot_col[:, 4 + 2 * layer + k : 5 + 2 * layer + k]
        out = out + jnp.where((lanes == named) & held, dg, 0.0)
        part = dot_nn(one_where(place_mask(slot_row, layer, k, slots)), (g[k] * dx2).astype(BF16))
        total = part if total is None else total + part
    dg_ref[...] = out
    send_ref[...] = total.astype(BF16).reshape(send_ref.shape)


def attention_back(layer, images, experts, dense_ref, slot_col, back_ref, dx2, dr, router, x, x1, c, o_ref, qkv_ref, a_ref, acc_ref, dqkv_ref, do_ref):
    toks, width = x.shape
    rows = toks // images
    slots = back_ref.shape[0] * back_ref.shape[1]
    router_rows, vec = dense_parts(dense_ref, experts)
    dlog = (router * (dr - jnp.sum(dr * router, axis=1, keepdims=True))).astype(BF16)
    pick = one_where(pick_mask(slot_col, layer, 0, slots) | pick_mask(slot_col, layer, 1, slots))
    dc = dot_nn(pick, back_ref[...].reshape(slots, width)) + dot_nn(dlog, router_rows)
    acc_ref[4 * width : 4 * width + experts, :] += dot_tn(dlog, c)[:experts]
    hat, scale2 = normalise(x1)
    dgain2 = jnp.sum(dc * hat, axis=0, keepdims=True)
    dshift2 = jnp.sum(dc, axis=0, keepdims=True)
    dx1 = dx2 + norm_back(dc * vec[6:7], hat, scale2)
    dz = dx1.astype(BF16)
    dbo = jnp.sum(dz.astype(F32), axis=0, keepdims=True)
    acc_ref[3 * width : 4 * width, :] += dot_tn(o_ref[...], dz)
    do_ref[...] = dot_nt(dz, dense_ref[3 * width : 4 * width, :]).astype(BF16)
    key_dead = lax.broadcasted_iota(jnp.int32, (rows, rows), 0) >= PATCHES
    scale = (width // HEADS) ** (-0.5)
    first = half_mask(rows, 0)
    for image in range(images):
        at = slice(image * rows, (image + 1) * rows)
        for pair in range(width // LANES):
            cut = slice(pair * LANES, (pair + 1) * LANES)
            q2 = qkv_ref[at, cut]
            k2 = qkv_ref[at, width + pair * LANES : width + (pair + 1) * LANES]
            v2 = qkv_ref[at, 2 * width + pair * LANES : 2 * width + (pair + 1) * LANES]
            do2 = do_ref[at, cut]
            dqs, dks, dvs = [], [], []
            for half in range(2):
                keep = half_mask(rows, half)
                q_half = jnp.where(keep, q2, jnp.zeros_like(q2))
                do_half = jnp.where(keep, do2, jnp.zeros_like(do2))
                s = jnp.where(key_dead, NEG_FILL, dot_nt(k2, q_half) * scale)
                e = jnp.exp(s - jnp.max(s, axis=0, keepdims=True))
                p = e * (1.0 / jnp.sum(e, axis=0, keepdims=True))
                dp = dot_nt(v2, do_half)
                ds = (p * (dp - jnp.sum(dp * p, axis=0, keepdims=True))).astype(BF16)
                dvs.append(dot_nn(p.astype(BF16), do2))
                dks.append(dot_nn(ds, q2))
                dqs.append(dot_tn(ds, k2))
            dqkv_ref[at, cut] = (jnp.where(first, dqs[0], dqs[1]) * scale).astype(BF16)
            dqkv_ref[at, width + pair * LANES : width + (pair + 1) * LANES] = (
                jnp.where(first, dks[0], dks[1]) * scale
            ).astype(BF16)
            dqkv_ref[at, 2 * width + pair * LANES : 2 * width + (pair + 1) * LANES] = jnp.where(
                first, dvs[0], dvs[1]
            ).astype(BF16)
    a = a_ref[...]
    da = None
    biases = []
    for part in range(3):
        at = slice(part * width, (part + 1) * width)
        dq = dqkv_ref[:, at]
        acc_ref[at, :] += dot_tn(dq, a)
        biases.append(jnp.sum(dq.astype(F32), axis=0, keepdims=True))
        piece = dot_nn(dq, dense_ref[at, :])
        da = piece if da is None else da + piece
    hat, scale1 = normalise(x)
    dgain1 = jnp.sum(da * hat, axis=0, keepdims=True)
    dshift1 = jnp.sum(da, axis=0, keepdims=True)
    acc_ref[4 * width + experts : 4 * width + experts + 8, :] += jnp.concatenate(
        [dgain1, dshift1, *biases, dbo, dgain2, dshift2], axis=0
    )
    return dx1 + norm_back(da * vec[0:1], hat, scale1)


def pack_rows(block, images, rows):
    each = block.shape[0] // images
    return jnp.concatenate([block[i * each : i * each + rows] for i in range(images)], axis=0)


def unpack_rows(packed, images, each):
    rows = packed.shape[0] // images
    fill = jnp.zeros((each - rows, packed.shape[1]), packed.dtype)
    parts = []
    for i in range(images):
        parts += [packed[i * rows : (i + 1) * rows], fill]
    return jnp.concatenate(parts, axis=0)


def first_kernel(sizes, tok_ref, dense_ref, col_ref, row_ref, *outs):
    images, rows, experts = sizes
    x_ref, qkv_ref, a_ref, o_ref, x1_ref, c_ref, router_ref, send_ref = outs
    x = pack_rows(tok_ref[...].astype(F32), images, rows)
    x_ref[...] = x
    attention_forward(x, 0, images, experts, dense_ref, col_ref[...], row_ref[...], qkv_ref, a_ref, o_ref, x1_ref, c_ref, router_ref, send_ref)


def middle_kernel(sizes, layer, back_ref, x1_old, router_old, dense_ref, col_ref, row_ref, picked_ref, *outs):
    images, rows, experts = sizes
    x_ref, qkv_ref, a_ref, o_ref, x1_ref, c_ref, router_ref, send_ref = outs
    x = combine(x1_old[...], router_old[...], col_ref[...], layer - 1, back_ref[...], picked_ref)
    x_ref[...] = x
    attention_forward(x, layer, images, experts, dense_ref, col_ref[...], row_ref[...], qkv_ref, a_ref, o_ref, x1_ref, c_ref, router_ref, send_ref)


def turn_kernel(sizes, layer, back_ref, x1_old, router_old, cot_ref, col_ref, row_ref, out_ref, dx_ref, dg_ref, send_ref, picked_ref):
    images, rows, experts = sizes
    each = out_ref.shape[0] // images
    col = col_ref[...]
    x = combine(x1_old[...], router_old[...], col, layer, back_ref[...], picked_ref)
    ok = col[:, 8:9] > 0
    out_ref[...] = unpack_rows(jnp.where(ok, x, 0.0), images, each)
    dx = jnp.where(ok, pack_rows(cot_ref[...].astype(F32), images, rows), 0.0)
    dx_ref[...] = dx
    combine_back(dx, router_old[...], col, row_ref[...], layer, picked_ref, dg_ref, send_ref)


def flush_dense(acc_ref, dense_out):
    @pl.when(pl.program_id(0) == pl.num_programs(0) - 1)
    def _():
        rows = dense_out.shape[1]
        shard = acc_ref.shape[0] // dense_out.shape[0]
        for at in range(dense_out.shape[0]):
            dense_out[at, :shard, :] = acc_ref[at * shard : (at + 1) * shard, :].astype(BF16)
            if rows > shard:
                dense_out[at, shard:, :] = jnp.zeros((rows - shard, acc_ref.shape[1]), BF16)


def back_common(sizes, layer, refs):
    images, rows, experts = sizes
    (back_ref, dx_ref, dg_ref, router_ref, x_ref, x1_ref, c_ref, o_ref, qkv_ref, a_ref, dense_ref, col_ref, acc_ref, dqkv_ref, do_ref) = refs

    @pl.when(pl.program_id(0) == 0)
    def _():
        acc_ref[...] = jnp.zeros_like(acc_ref)

    return attention_back(layer, images, experts, dense_ref, col_ref[...], back_ref, dx_ref[...], dg_ref[...], router_ref[...], x_ref[...], x1_ref[...], c_ref[...], o_ref, qkv_ref, a_ref, acc_ref, dqkv_ref, do_ref)


def back_kernel(sizes, layer, *refs):
    (back_ref, dx_ref, dg_ref, router_ref, x_ref, x1_ref, c_ref, o_ref, qkv_ref, a_ref, dense_ref, col_ref, row_ref, router_low, picked_low, dx_out, dg_out, send_ref, dense_out, acc_ref, dqkv_ref, do_ref) = refs
    dx = back_common(sizes, layer, (back_ref, dx_ref, dg_ref, router_ref, x_ref, x1_ref, c_ref, o_ref, qkv_ref, a_ref, dense_ref, col_ref, acc_ref, dqkv_ref, do_ref))
    dx_out[...] = dx
    combine_back(dx, router_low[...], col_ref[...], row_ref[...], layer - 1, picked_low, dg_out, send_ref)
    flush_dense(acc_ref, dense_out)


def last_kernel(sizes, *refs):
    (back_ref, dx_ref, dg_ref, router_ref, x_ref, x1_ref, c_ref, o_ref, qkv_ref, a_ref, dense_ref, col_ref, dx_out, dense_out, acc_ref, dqkv_ref, do_ref) = refs
    dx = back_common(sizes, 0, (back_ref, dx_ref, dg_ref, router_ref, x_ref, x1_ref, c_ref, o_ref, qkv_ref, a_ref, dense_ref, col_ref, acc_ref, dqkv_ref, do_ref))
    dx_out[...] = unpack_rows(dx, sizes[0], dx_out.shape[0] // sizes[0])
    flush_dense(acc_ref, dense_out)


class Shapes:
    def __init__(self, micros, images, rows, each, width, hidden, experts, slots_each, dense_rows, shards):
        self.micros, self.images, self.rows, self.each = micros, images, rows, each
        self.width, self.hidden, self.experts, self.slots_each = width, hidden, experts, slots_each
        self.dense_rows, self.shards = dense_rows, shards
        self.toks = images * rows
        self.sizes = (images, rows, experts)

    def per_micro(self, *shape, dtype=F32):
        full = (self.micros, *shape)
        spec = pl.BlockSpec((None, *shape), lambda m: (m, *([0] * len(shape))))
        return spec, jax.ShapeDtypeStruct(full, dtype)

    def exchange(self):
        full = (self.experts, self.micros, self.slots_each, self.width)
        spec = pl.BlockSpec((self.experts, None, self.slots_each, self.width), lambda m: (0, m, 0, 0))
        return spec, jax.ShapeDtypeStruct(full, BF16)

    def token_block(self, dtype):
        per = self.images * self.each
        return pl.BlockSpec((per, self.width), lambda m: (m, 0)), jax.ShapeDtypeStruct((self.micros * per, self.width), dtype)

    def whole(self, *shape, dtype=BF16):
        spec = pl.BlockSpec(shape, lambda m: (0,) * len(shape), pipeline_mode=pl.Buffered(1))
        return spec, jax.ShapeDtypeStruct(shape, dtype)

    def forward_outs(self):
        t, w = self.toks, self.width
        return [
            self.per_micro(t, w),
            self.per_micro(t, 3 * w, dtype=BF16),
            self.per_micro(t, w, dtype=BF16),
            self.per_micro(t, w, dtype=BF16),
            self.per_micro(t, w),
            self.per_micro(t, w, dtype=BF16),
            self.per_micro(t, LANES),
            self.exchange(),
        ]

    def picked(self):
        return self.per_micro(2, self.toks, self.width, dtype=BF16)

    def cols(self):
        return self.per_micro(self.toks, LANES, dtype=jnp.int32)

    def row(self):
        return self.per_micro(8, self.toks, dtype=jnp.int32)

    def dense(self):
        return self.whole(self.dense_rows, self.width)

    def dense_out(self):
        return self.whole(self.shards, up_to(self.dense_rows // self.shards, 16), self.width)

    def scratch(self):
        return [
            pltpu.VMEM((self.dense_rows, self.width), F32),
            pltpu.VMEM((self.toks, 3 * self.width), BF16),
            pltpu.VMEM((self.toks, self.width), BF16),
        ]

    def saved_ins(self):
        t, w = self.toks, self.width
        return [self.exchange(), self.per_micro(t, w), self.per_micro(t, LANES), self.per_micro(t, LANES)] + self.forward_outs()[0:1] + [
            self.per_micro(t, w),
            self.per_micro(t, w, dtype=BF16),
            self.per_micro(t, w, dtype=BF16),
            self.per_micro(t, 3 * w, dtype=BF16),
            self.per_micro(t, w, dtype=BF16),
            self.dense(),
            self.cols(),
        ]

    def call(self, kernel, ins, outs, args, name, scratch=()):
        return pl.pallas_call(
            kernel,
            grid=(self.micros,),
            in_specs=[spec for spec, _ in ins],
            out_specs=[spec for spec, _ in outs],
            out_shape=[shape for _, shape in outs],
            scratch_shapes=list(scratch),
            compiler_params=pltpu.CompilerParams(vmem_limit_bytes=VMEM_LIMIT),
            name=name,
        )(*args)


def first_stage(shp, tokens, dense, cols, rows):
    return shp.call(
        functools.partial(first_kernel, shp.sizes),
        [shp.token_block(BF16), shp.dense(), shp.cols(), shp.row()],
        shp.forward_outs(),
        (tokens, dense, cols, rows),
        "attn_first",
    )


def middle_stage(shp, layer, back, x1, router, dense, cols, rows):
    t, w = shp.toks, shp.width
    return shp.call(
        functools.partial(middle_kernel, shp.sizes, layer),
        [shp.exchange(), shp.per_micro(t, w), shp.per_micro(t, LANES), shp.dense(), shp.cols(), shp.row()],
        [shp.picked(), *shp.forward_outs()],
        (back, x1, router, dense, cols, rows),
        "attn_next",
    )


def turn_stage(shp, layer, back, x1, router, cotangent, cols, rows):
    t, w = shp.toks, shp.width
    return shp.call(
        functools.partial(turn_kernel, shp.sizes, layer),
        [shp.exchange(), shp.per_micro(t, w), shp.per_micro(t, LANES), shp.token_block(BF16), shp.cols(), shp.row()],
        [shp.token_block(F32), shp.per_micro(t, w), shp.per_micro(t, LANES), shp.exchange()],
        (back, x1, router, cotangent, cols, rows),
        "turn",
        scratch=[pltpu.VMEM((2, t, w), BF16)],
    )


def back_stage(shp, layer, back, dx, dg, saved, dense, cols, rows, router_low, picked_low):
    t, w = shp.toks, shp.width
    x, qkv, a, o, x1, c, router = saved
    return shp.call(
        functools.partial(back_kernel, shp.sizes, layer),
        [*shp.saved_ins(), shp.row(), shp.per_micro(t, LANES), shp.picked()],
        [shp.per_micro(t, w), shp.per_micro(t, LANES), shp.exchange(), shp.dense_out()],
        (back, dx, dg, router, x, x1, c, o, qkv, a, dense, cols, rows, router_low, picked_low),
        "attn_back",
        scratch=shp.scratch(),
    )


def last_stage(shp, back, dx, dg, saved, dense, cols):
    x, qkv, a, o, x1, c, router = saved
    return shp.call(
        functools.partial(last_kernel, shp.sizes),
        shp.saved_ins(),
        [shp.token_block(F32), shp.dense_out()],
        (back, dx, dg, router, x, x1, c, o, qkv, a, dense, cols),
        "attn_last",
        scratch=shp.scratch(),
    )


def gelu_parts(h):
    cdf = 0.5 * (1.0 + lax.erf(h * INV_SQRT2))
    slope = cdf + h * (INV_SQRT2PI * jnp.exp(-0.5 * (h * h)))
    return (h * cdf).astype(BF16), slope.astype(BF16)


def expert_forward_kernel(x_ref, mats_ref, shift_ref, y_ref, act_ref, slope_ref):
    width, hidden = x_ref.shape[1], mats_ref.shape[1]
    shift = shift_ref[...].astype(F32)
    y = None
    for at in range(0, hidden, 512):
        cut = slice(at, at + 512)
        h = dot_nn(x_ref[...], mats_ref[:width, cut]) + shift[:, cut]
        act, slope = gelu_parts(h)
        act_ref[:, cut] = act
        slope_ref[:, cut] = slope
        piece = dot_nt(act, mats_ref[width:, cut])
        y = piece if y is None else y + piece
    y_ref[...] = (y + shift[:, hidden:]).astype(BF16)


def expert_forward(x, mats, shift):
    rows, width = x.shape
    hidden = mats.shape[1]
    block = 256
    return pl.pallas_call(
        expert_forward_kernel,
        grid=(rows // block,),
        in_specs=[
            pl.BlockSpec((block, width), lambda r: (r, 0)),
            pl.BlockSpec(mats.shape, lambda r: (0, 0), pipeline_mode=pl.Buffered(1)),
            pl.BlockSpec(shift.shape, lambda r: (0, 0)),
        ],
        out_specs=[
            pl.BlockSpec((block, width), lambda r: (r, 0)),
            pl.BlockSpec((block, hidden), lambda r: (r, 0)),
            pl.BlockSpec((block, hidden), lambda r: (r, 0)),
        ],
        out_shape=[
            jax.ShapeDtypeStruct((rows, width), BF16),
            jax.ShapeDtypeStruct((rows, hidden), BF16),
            jax.ShapeDtypeStruct((rows, hidden), BF16),
        ],
        compiler_params=pltpu.CompilerParams(vmem_limit_bytes=VMEM_LIMIT),
        name="expert_forward",
    )(x, mats, shift)


def expert_back_kernel(dy_ref, x_ref, act_ref, slope_ref, w_in_ref, w_out_ref, dx_ref, dw_ref, db_ref, xt_ref, dyt_ref, total_ref):
    step = pl.program_id(0)
    width = x_ref.shape[1]

    @pl.when(step == 0)
    def _():
        xt_ref[...] = x_ref[...].T
        dyt_ref[...] = dy_ref[...].T
        total_ref[...] = jnp.zeros_like(total_ref)

    dh = (dot_nn(dy_ref[...], w_out_ref[...]) * slope_ref[...].astype(F32)).astype(BF16)
    db_ref[...] = jnp.sum(dh.astype(F32), axis=0, keepdims=True)
    dw_ref[:width, :] = dot_nn(xt_ref[...], dh).astype(BF16)
    dw_ref[width:, :] = dot_nn(dyt_ref[...], act_ref[...]).astype(BF16)
    total_ref[...] += dot_nt(dh, w_in_ref[...])

    @pl.when(step == pl.num_programs(0) - 1)
    def _():
        dx_ref[...] = total_ref[...].astype(BF16)


def expert_back(dy, x, act, slope, mats):
    rows, width = x.shape
    hidden = mats.shape[1]
    block = 256
    full = lambda f: (0, 0)
    return pl.pallas_call(
        expert_back_kernel,
        grid=(hidden // block,),
        in_specs=[
            pl.BlockSpec((rows, width), full, pipeline_mode=pl.Buffered(1)),
            pl.BlockSpec((rows, width), full, pipeline_mode=pl.Buffered(1)),
            pl.BlockSpec((rows, block), lambda f: (0, f)),
            pl.BlockSpec((rows, block), lambda f: (0, f)),
            pl.BlockSpec((width, block), lambda f: (0, f)),
            pl.BlockSpec((width, block), lambda f: (1, f)),
        ],
        out_specs=[
            pl.BlockSpec((rows, width), full, pipeline_mode=pl.Buffered(1)),
            pl.BlockSpec((2 * width, block), lambda f: (0, f)),
            pl.BlockSpec((1, block), lambda f: (0, f)),
        ],
        out_shape=[
            jax.ShapeDtypeStruct((rows, width), BF16),
            jax.ShapeDtypeStruct((2 * width, hidden), BF16),
            jax.ShapeDtypeStruct((1, hidden), F32),
        ],
        scratch_shapes=[
            pltpu.VMEM((width, rows), BF16),
            pltpu.VMEM((width, rows), BF16),
            pltpu.VMEM((rows, width), F32),
        ],
        compiler_params=pltpu.CompilerParams(vmem_limit_bytes=VMEM_LIMIT),
        name="expert_back",
    )(dy, x, act, slope, mats, mats)


def adam_update(master, first_mom, second_mom, gradient, clip_scale, step_float):
    clipped = gradient * clip_scale
    first_new = BETA_ONE * first_mom + (1.0 - BETA_ONE) * clipped
    second_new = BETA_TWO * second_mom + (1.0 - BETA_TWO) * clipped * clipped
    first_hat = first_new / (1.0 - BETA_ONE**step_float)
    second_hat = second_new / (1.0 - BETA_TWO**step_float)
    change = -STEP_RATE * (first_hat / (jnp.sqrt(second_hat) + ADAM_EPS) + DECAY_RATE * master)
    return (change, first_new, second_new)


def local(
    tokens,
    cotangent,
    valid,
    routes,
    priority,
    step,
    dense_master,
    dense_first,
    dense_second,
    expert_master,
    expert_first,
    expert_second,
    shift_master,
    shift_first,
    shift_second,
):
    layer_count, shard_rows, width = dense_master.shape
    micros, group_tok = priority.shape
    each = valid.shape[1]
    images = group_tok // each
    hidden = expert_master.shape[3]
    groups = lax.axis_size("expert")
    shards = lax.axis_size("dp")
    experts = expert_master.shape[1] * groups
    capacity = (9 * images * PATCHES + 4 * experts - 1) // (4 * experts)
    slots_each = up_to(capacity, 16)
    rows = up_to(PATCHES, 16)
    shp = Shapes(micros, images, rows, each, width, hidden, experts, slots_each, shard_rows * shards, shards)

    dense_low = dense_master.astype(BF16)
    dense = [lax.all_gather(dense_low[i], "dp", axis=0, tiled=True) for i in range(layer_count)]
    expert_low = expert_master.astype(BF16)
    shift_low = shift_master.astype(BF16)
    mats = [lax.all_gather(expert_low[i, 0], "dp", axis=0, tiled=True) for i in range(layer_count)]
    shift = lax.all_gather(shift_low, "dp", axis=2, tiled=True)

    def cut(values):
        return values.reshape(micros, images, each)[:, :, :rows].reshape(micros, images * rows)

    planes = [cut(priority), cut(valid)]
    for i in range(layer_count):
        planes += [cut(routes[i, :, 0]), cut(routes[i, :, 1])]
    planes += [jnp.zeros_like(planes[0])] * (8 - len(planes))
    meta = jnp.stack(planes, axis=1)
    slot_col, slot_row = routing(meta, jnp.swapaxes(meta, 1, 2), capacity, slots_each, experts, layer_count)

    def exchange(values):
        return lax.all_to_all(values, "expert", split_axis=0, concat_axis=0, tiled=True)

    flat = (experts * micros * slots_each, width)
    saved, kept, picks = [], [], []
    for i in range(layer_count):
        if i == 0:
            outs = first_stage(shp, tokens, dense[0], slot_col, slot_row)
        else:
            picked, *outs = middle_stage(shp, i, back, saved[i - 1][4], saved[i - 1][6], dense[i], slot_col, slot_row)
            picks.append(picked)
        *state, send = outs
        saved.append(state)
        received = exchange(send).reshape(flat)
        produced, act, slope = expert_forward(received, mats[i], shift[i])
        kept.append((received, act, slope))
        back = exchange(produced.reshape(send.shape))
    top = layer_count - 1
    output, dx, dg, send = turn_stage(shp, top, back, saved[top][4], saved[top][6], cotangent, slot_col, slot_row)
    dense_grads, mats_grads, shift_grads = [None] * layer_count, [None] * layer_count, [None] * layer_count
    for i in reversed(range(layer_count)):
        received, act, slope = kept[i]
        dy = exchange(send).reshape(flat)
        dsent, dmats, dshift_in = expert_back(dy, received, act, slope, mats[i])
        mats_grads[i] = dmats
        shift_grads[i] = jnp.concatenate([dshift_in[0], jnp.sum(dy, axis=0, dtype=F32)])
        back = exchange(dsent.reshape(send.shape))
        if i:
            dx, dg, send, dense_grads[i] = back_stage(
                shp, i, back, dx, dg, saved[i], dense[i], slot_col, slot_row, saved[i - 1][6], picks[i - 1]
            )
        else:
            grad_tokens, dense_grads[i] = last_stage(shp, back, dx, dg, saved[i], dense[i], slot_col)
    dense_parts_sum = [
        lax.psum(lax.psum_scatter(g, "dp", scatter_dimension=0, tiled=False), "expert") for g in dense_grads
    ]
    dense_shard = jnp.stack([g[:shard_rows] for g in dense_parts_sum]).astype(F32)
    expert_shard = jnp.stack(
        [lax.psum_scatter(g, "dp", scatter_dimension=0, tiled=True) for g in mats_grads]
    ).astype(F32)[:, None]
    shift_shard = lax.psum_scatter(
        jnp.stack(shift_grads)[:, None].astype(BF16), "dp", scatter_dimension=2, tiled=True
    ).astype(F32)
    first_replica = (lax.axis_index("expert") == 0).astype(F32)
    square = (
        jnp.sum(dense_shard * dense_shard) * first_replica
        + jnp.sum(expert_shard * expert_shard)
        + jnp.sum(shift_shard * shift_shard)
    )
    grad_norm = jnp.sqrt(lax.psum(square, ("dp", "expert")))
    clip_scale = CLIP_NORM / jnp.maximum(grad_norm, CLIP_NORM)
    step_float = step.astype(F32)
    dense_new = adam_update(dense_master, dense_first, dense_second, dense_shard, clip_scale, step_float)
    expert_new = adam_update(expert_master, expert_first, expert_second, expert_shard, clip_scale, step_float)
    shift_new = adam_update(shift_master, shift_first, shift_second, shift_shard, clip_scale, step_float)
    return (output, grad_tokens, grad_norm, dense_shard, *dense_new, expert_shard, *expert_new, shift_shard, *shift_new)


def solution(mesh):
    split = P(("dp", "expert"), None)
    dense = P(None, "dp", None)
    mats = P(None, "expert", "dp", None)
    shift = P(None, "expert", "dp")
    placed = (split, split, split, P(None, ("dp", "expert"), None), split, P()) + (dense,) * 3 + (mats,) * 3 + (shift,) * 3
    return jax.shard_map(
        local,
        mesh=mesh,
        in_specs=placed,
        out_specs=(split, split, P()) + (dense,) * 4 + (mats,) * 4 + (shift,) * 4,
        check_vma=False,
    )
```

```python
import functools

import jax
import jax.numpy as jnp
from jax import lax
from jax.experimental import pallas as pl
from jax.experimental.pallas import tpu as pltpu
from jax.sharding import PartitionSpec as P

HEADS = 8
PATCHES = 197


NORM_EPS = 1e-06
NEG_FILL = -1e30
CLIP_NORM = 1.0
BETA_ONE = 0.9
BETA_TWO = 0.95
STEP_RATE = 0.01
DECAY_RATE = 0.1
ADAM_EPS = 1e-08
LANES = 128
MESH = pl.DeviceIdType.MESH
VMEM_LIMIT = 60 * 1024 * 1024
F32 = jnp.float32
BF16 = jnp.bfloat16
INV_SQRT2 = 0.7071067811865476
INV_SQRT2PI = 0.3989422804014327


def up_to(count, step):
    return -(-count // step) * step


def dot_nn(left, right):
    return lax.dot_general(left, right, (((1,), (0,)), ((), ())), preferred_element_type=F32)


def dot_nt(left, right):
    return lax.dot_general(left, right, (((1,), (1,)), ((), ())), preferred_element_type=F32)


def dot_tn(left, right):
    return lax.dot_general(left, right, (((0,), (0,)), ((), ())), preferred_element_type=F32)


def lane_ids(rows, cols=LANES):
    return lax.broadcasted_iota(jnp.int32, (rows, cols), 1)


def one_where(mask):
    return jnp.where(mask, 1.0, 0.0).astype(BF16)


def normalise(values):
    centred = values - jnp.mean(values, axis=-1, keepdims=True)
    spread = jnp.mean(centred * centred, axis=-1, keepdims=True)
    scale = lax.rsqrt(spread + NORM_EPS)
    return centred * scale, scale


def norm_back(grad_hat, hat, scale):
    return scale * (
        grad_hat
        - jnp.mean(grad_hat, axis=-1, keepdims=True)
        - hat * jnp.mean(grad_hat * hat, axis=-1, keepdims=True)
    )


def dense_parts(dense_ref, experts):
    width = dense_ref.shape[-1]
    tail = dense_ref[4 * width :, :].astype(F32)
    vectors = tail[experts : experts + 8]
    router_rows = jnp.concatenate(
        [tail[:experts], jnp.zeros((LANES - experts, width), F32)], axis=0
    ).astype(BF16)
    return router_rows, vectors


def cost(us):
    return pl.CostEstimate(flops=int(us * 1.0e9), bytes_accessed=int(us * 3.0e6), transcendentals=0)


def routing_kernel(capacity, slots_each, experts, rows, priority_ref, valid_ref, routes_ref, slot_col_ref, slot_row_ref):
    micro = pl.program_id(0)
    layers, _, group = routes_ref.shape
    images = valid_ref.shape[0] // priority_ref.shape[0]
    each = valid_ref.shape[1]
    lines = [priority_ref[pl.ds(micro, 1), :]]
    lines.append(jnp.concatenate([valid_ref[pl.ds(micro * images + i, 1), :] for i in range(images)], axis=1))
    for layer in range(layers):
        for k in range(2):
            lines.append(routes_ref[layer, k : k + 1, :])
    subs = lax.broadcasted_iota(jnp.int32, (LANES, group), 0)
    table = jnp.zeros((LANES, group), F32)
    for at, line in enumerate(lines):
        table = jnp.where(subs == at, line.astype(F32), table)
    cols = table.T

    def packed(column):
        return jnp.concatenate([column[i * each : i * each + rows] for i in range(images)], axis=0)

    mine = packed(cols)
    toks = images * rows
    before = one_where(lines[0].astype(F32) < mine[:, 0:1])
    ok_all, ok_mine = cols[:, 1:2] > 0.0, mine[:, 1:2] > 0.0
    labels = lane_ids(1).astype(F32)
    lanes = lane_ids(toks)
    full = jnp.where(lanes == 8, mine[:, 1:2], 0.0)
    for layer in range(layers):
        firsts = 0.0
        for k in range(2):
            at = 2 + 2 * layer + k
            hot = one_where((cols[:, at : at + 1] == labels) & ok_all)
            counts = dot_nn(before, hot) + firsts
            firsts = jnp.sum(hot.astype(F32), axis=0, keepdims=True)
            named = mine[:, at : at + 1]
            place = jnp.sum(jnp.where(named == labels, counts, 0.0), axis=1, keepdims=True)
            slot = jnp.where((place < capacity) & ok_mine, named * slots_each + place, -1.0)
            full = jnp.where(lanes == 2 * layer + k, slot, full)
            full = jnp.where(lanes == 4 + 2 * layer + k, named, full)
    slot_col_ref[...] = full.astype(jnp.int32)
    fill = up_to(toks, LANES) - toks
    turned = jnp.concatenate([full, jnp.zeros((fill, LANES), F32)], axis=0).T
    slot_row_ref[...] = turned[:8, :toks].astype(jnp.int32)


def routing(priority, valid, routes, capacity, slots_each, experts, rows):
    micros, group = priority.shape
    images = valid.shape[0] // micros
    layers = routes.shape[0]
    toks = images * rows
    return pl.pallas_call(
        functools.partial(routing_kernel, capacity, slots_each, experts, rows),
        grid=(micros,),
        in_specs=[
            pl.BlockSpec(priority.shape, lambda m: (0, 0)),
            pl.BlockSpec(valid.shape, lambda m: (0, 0)),
            pl.BlockSpec((layers, 2, group), lambda m: (0, 0, m)),
        ],
        out_specs=[
            pl.BlockSpec((None, toks, LANES), lambda m: (m, 0, 0)),
            pl.BlockSpec((None, 8, toks), lambda m: (m, 0, 0)),
        ],
        out_shape=[
            jax.ShapeDtypeStruct((micros, toks, LANES), jnp.int32),
            jax.ShapeDtypeStruct((micros, 8, toks), jnp.int32),
        ],
        compiler_params=pltpu.CompilerParams(vmem_limit_bytes=VMEM_LIMIT),
        cost_estimate=cost(5),
        name="routing",
    )(priority, valid, routes)


def gates(router, slot_col, layer):
    lanes = lane_ids(router.shape[0])
    out = []
    for k in range(2):
        named = slot_col[:, 4 + 2 * layer + k : 5 + 2 * layer + k]
        value = jnp.sum(jnp.where(lanes == named, router, 0.0), axis=1, keepdims=True)
        held = slot_col[:, 2 * layer + k : 2 * layer + k + 1] >= 0
        out.append(jnp.where(held, value, 0.0))
    return out


def pick_mask(slot_col, layer, k, slots):
    toks = slot_col.shape[0]
    return lax.broadcasted_iota(jnp.int32, (toks, slots), 1) == slot_col[:, 2 * layer + k : 2 * layer + k + 1]


def place_mask(slot_row, layer, k, slots):
    toks = slot_row.shape[1]
    return lax.broadcasted_iota(jnp.int32, (slots, toks), 0) == slot_row[2 * layer + k : 2 * layer + k + 1]


def half_mask(rows, half):
    lanes = lane_ids(rows)
    return (lanes >= LANES // 2) if half else (lanes < LANES // 2)


def attention_forward(x, layer, images, experts, dense_ref, slot_col, slot_row, qkv_ref, a_ref, o_ref, x1_ref, c_ref, router_ref, send_ref):
    toks, width = x.shape
    rows = toks // images
    router_rows, vec = dense_parts(dense_ref, experts)
    hat, _ = normalise(x)
    a = (hat * vec[0:1] + vec[1:2]).astype(BF16)
    a_ref[...] = a
    for part in range(3):
        at = slice(part * width, (part + 1) * width)
        qkv_ref[:, at] = (dot_nt(a, dense_ref[at, :]) + vec[2 + part : 3 + part]).astype(BF16)
    key_dead = lane_ids(rows, rows) >= PATCHES
    scale = (width // HEADS) ** (-0.5)
    for image in range(images):
        at = slice(image * rows, (image + 1) * rows)
        for pair in range(width // LANES):
            q2 = qkv_ref[at, pair * LANES : (pair + 1) * LANES]
            k2 = qkv_ref[at, width + pair * LANES : width + (pair + 1) * LANES]
            v2 = qkv_ref[at, 2 * width + pair * LANES : 2 * width + (pair + 1) * LANES]
            both = []
            for half in range(2):
                q_half = jnp.where(half_mask(rows, half), q2, jnp.zeros_like(q2))
                s = jnp.where(key_dead, NEG_FILL, dot_nt(q_half, k2) * scale)
                e = jnp.exp(s - jnp.max(s, axis=1, keepdims=True))
                p = e * (1.0 / jnp.sum(e, axis=1, keepdims=True))
                both.append(dot_nn(p.astype(BF16), v2))
            o2 = jnp.where(half_mask(rows, 0), both[0], both[1])
            o_ref[at, pair * LANES : (pair + 1) * LANES] = o2.astype(BF16)
    x1 = x + (dot_nn(o_ref[...], dense_ref[3 * width : 4 * width, :]) + vec[5:6])
    x1_ref[...] = x1
    hat, _ = normalise(x1)
    c = (hat * vec[6:7] + vec[7:8]).astype(BF16)
    c_ref[...] = c
    logits = jnp.where(lane_ids(toks) < experts, dot_nt(c, router_rows), NEG_FILL)
    e = jnp.exp(logits - jnp.max(logits, axis=1, keepdims=True))
    router_ref[...] = e / jnp.sum(e, axis=1, keepdims=True)
    slots = send_ref.shape[0] * send_ref.shape[1]
    place = one_where(place_mask(slot_row, layer, 0, slots) | place_mask(slot_row, layer, 1, slots))
    send_ref[...] = dot_nn(place, c).astype(BF16).reshape(send_ref.shape)


def combine(x1, router, slot_col, layer, back, picked_ref):
    slots = back.shape[0] * back.shape[1]
    y = back.reshape(slots, back.shape[2])
    g = gates(router, slot_col, layer)
    total = x1
    for k in range(2):
        picked = dot_nn(one_where(pick_mask(slot_col, layer, k, slots)), y)
        picked_ref[k] = picked.astype(BF16)
        total = total + g[k] * picked
    return total


def combine_back(dx2, router, slot_col, slot_row, layer, picked_ref, dg_ref, send_ref):
    slots = send_ref.shape[0] * send_ref.shape[1]
    toks = dx2.shape[0]
    g = gates(router, slot_col, layer)
    lanes = lane_ids(toks)
    out = jnp.zeros((toks, LANES), F32)
    total = None
    for k in range(2):
        held = slot_col[:, 2 * layer + k : 2 * layer + k + 1] >= 0
        dg = jnp.sum(dx2 * picked_ref[k].astype(F32), axis=1, keepdims=True)
        named = slot_col[:, 4 + 2 * layer + k : 5 + 2 * layer + k]
        out = out + jnp.where((lanes == named) & held, dg, 0.0)
        part = dot_nn(one_where(place_mask(slot_row, layer, k, slots)), (g[k] * dx2).astype(BF16))
        total = part if total is None else total + part
    dg_ref[...] = out
    send_ref[...] = total.astype(BF16).reshape(send_ref.shape)


def attention_back(layer, images, experts, dense_ref, slot_col, back_ref, dx2, dr, router, x, x1, c, o_ref, qkv_ref, a_ref, acc_ref, dqkv_ref, do_ref):
    toks, width = x.shape
    rows = toks // images
    slots = back_ref.shape[0] * back_ref.shape[1]
    router_rows, vec = dense_parts(dense_ref, experts)
    dlog = (router * (dr - jnp.sum(dr * router, axis=1, keepdims=True))).astype(BF16)
    pick = one_where(pick_mask(slot_col, layer, 0, slots) | pick_mask(slot_col, layer, 1, slots))
    dc = dot_nn(pick, back_ref[...].reshape(slots, width)) + dot_nn(dlog, router_rows)
    acc_ref[4 * width : 4 * width + experts, :] += dot_tn(dlog, c)[:experts]
    hat, scale2 = normalise(x1)
    dgain2 = jnp.sum(dc * hat, axis=0, keepdims=True)
    dshift2 = jnp.sum(dc, axis=0, keepdims=True)
    dx1 = dx2 + norm_back(dc * vec[6:7], hat, scale2)
    dz = dx1.astype(BF16)
    dbo = jnp.sum(dz.astype(F32), axis=0, keepdims=True)
    acc_ref[3 * width : 4 * width, :] += dot_tn(o_ref[...], dz)
    do_ref[...] = dot_nt(dz, dense_ref[3 * width : 4 * width, :]).astype(BF16)
    key_dead = lax.broadcasted_iota(jnp.int32, (rows, rows), 0) >= PATCHES
    scale = (width // HEADS) ** (-0.5)
    first = half_mask(rows, 0)
    for image in range(images):
        at = slice(image * rows, (image + 1) * rows)
        for pair in range(width // LANES):
            cut = slice(pair * LANES, (pair + 1) * LANES)
            q2 = qkv_ref[at, cut]
            k2 = qkv_ref[at, width + pair * LANES : width + (pair + 1) * LANES]
            v2 = qkv_ref[at, 2 * width + pair * LANES : 2 * width + (pair + 1) * LANES]
            do2 = do_ref[at, cut]
            dqs, dks, dvs = [], [], []
            for half in range(2):
                keep = half_mask(rows, half)
                q_half = jnp.where(keep, q2, jnp.zeros_like(q2))
                do_half = jnp.where(keep, do2, jnp.zeros_like(do2))
                s = jnp.where(key_dead, NEG_FILL, dot_nt(k2, q_half) * scale)
                e = jnp.exp(s - jnp.max(s, axis=0, keepdims=True))
                p = e * (1.0 / jnp.sum(e, axis=0, keepdims=True))
                dp = dot_nt(v2, do_half)
                ds = (p * (dp - jnp.sum(dp * p, axis=0, keepdims=True))).astype(BF16)
                dvs.append(dot_nn(p.astype(BF16), do2))
                dks.append(dot_nn(ds, q2))
                dqs.append(dot_tn(ds, k2))
            dqkv_ref[at, cut] = (jnp.where(first, dqs[0], dqs[1]) * scale).astype(BF16)
            dqkv_ref[at, width + pair * LANES : width + (pair + 1) * LANES] = (
                jnp.where(first, dks[0], dks[1]) * scale
            ).astype(BF16)
            dqkv_ref[at, 2 * width + pair * LANES : 2 * width + (pair + 1) * LANES] = jnp.where(
                first, dvs[0], dvs[1]
            ).astype(BF16)
    a = a_ref[...]
    da = None
    biases = []
    for part in range(3):
        at = slice(part * width, (part + 1) * width)
        dq = dqkv_ref[:, at]
        acc_ref[at, :] += dot_tn(dq, a)
        biases.append(jnp.sum(dq.astype(F32), axis=0, keepdims=True))
        piece = dot_nn(dq, dense_ref[at, :])
        da = piece if da is None else da + piece
    hat, scale1 = normalise(x)
    dgain1 = jnp.sum(da * hat, axis=0, keepdims=True)
    dshift1 = jnp.sum(da, axis=0, keepdims=True)
    acc_ref[4 * width + experts : 4 * width + experts + 8, :] += jnp.concatenate(
        [dgain1, dshift1, *biases, dbo, dgain2, dshift2], axis=0
    )
    return dx1 + norm_back(da * vec[0:1], hat, scale1)


def pack_rows(block, images, rows):
    each = block.shape[0] // images
    return jnp.concatenate([block[i * each : i * each + rows] for i in range(images)], axis=0)


def unpack_rows(packed, images, each):
    rows = packed.shape[0] // images
    fill = jnp.zeros((each - rows, packed.shape[1]), packed.dtype)
    parts = []
    for i in range(images):
        parts += [packed[i * rows : (i + 1) * rows], fill]
    return jnp.concatenate(parts, axis=0)


def first_kernel(sizes, tok_ref, dense_ref, col_ref, row_ref, *outs):
    images, rows, experts = sizes
    x_ref, qkv_ref, a_ref, o_ref, x1_ref, c_ref, router_ref, send_ref = outs
    x = pack_rows(tok_ref[...].astype(F32), images, rows)
    x_ref[...] = x
    attention_forward(x, 0, images, experts, dense_ref, col_ref[...], row_ref[...], qkv_ref, a_ref, o_ref, x1_ref, c_ref, router_ref, send_ref)


def middle_kernel(sizes, layer, back_ref, x1_old, router_old, dense_ref, col_ref, row_ref, picked_ref, *outs):
    images, rows, experts = sizes
    x_ref, qkv_ref, a_ref, o_ref, x1_ref, c_ref, router_ref, send_ref = outs
    x = combine(x1_old[...], router_old[...], col_ref[...], layer - 1, back_ref[...], picked_ref)
    x_ref[...] = x
    attention_forward(x, layer, images, experts, dense_ref, col_ref[...], row_ref[...], qkv_ref, a_ref, o_ref, x1_ref, c_ref, router_ref, send_ref)


def turn_kernel(sizes, layer, back_ref, x1_old, router_old, cot_ref, col_ref, row_ref, out_ref, dx_ref, dg_ref, send_ref, picked_ref):
    images, rows, experts = sizes
    each = out_ref.shape[0] // images
    col = col_ref[...]
    x = combine(x1_old[...], router_old[...], col, layer, back_ref[...], picked_ref)
    ok = col[:, 8:9] > 0
    out_ref[...] = unpack_rows(jnp.where(ok, x, 0.0), images, each)
    dx = jnp.where(ok, pack_rows(cot_ref[...].astype(F32), images, rows), 0.0)
    dx_ref[...] = dx
    combine_back(dx, router_old[...], col, row_ref[...], layer, picked_ref, dg_ref, send_ref)


def flush_dense(acc_ref, dense_out):
    @pl.when(pl.program_id(0) == pl.num_programs(0) - 1)
    def _():
        rows = dense_out.shape[1]
        shard = acc_ref.shape[0] // dense_out.shape[0]
        for at in range(dense_out.shape[0]):
            dense_out[at, :shard, :] = acc_ref[at * shard : (at + 1) * shard, :].astype(BF16)
            if rows > shard:
                dense_out[at, shard:, :] = jnp.zeros((rows - shard, acc_ref.shape[1]), BF16)


def back_common(sizes, layer, refs):
    images, rows, experts = sizes
    (back_ref, dx_ref, dg_ref, router_ref, x_ref, x1_ref, c_ref, o_ref, qkv_ref, a_ref, dense_ref, col_ref, acc_ref, dqkv_ref, do_ref) = refs

    @pl.when(pl.program_id(0) == 0)
    def _():
        acc_ref[...] = jnp.zeros_like(acc_ref)

    return attention_back(layer, images, experts, dense_ref, col_ref[...], back_ref, dx_ref[...], dg_ref[...], router_ref[...], x_ref[...], x1_ref[...], c_ref[...], o_ref, qkv_ref, a_ref, acc_ref, dqkv_ref, do_ref)


def back_kernel(sizes, layer, *refs):
    (back_ref, dx_ref, dg_ref, router_ref, x_ref, x1_ref, c_ref, o_ref, qkv_ref, a_ref, dense_ref, col_ref, row_ref, router_low, picked_low, dx_out, dg_out, send_ref, dense_out, acc_ref, dqkv_ref, do_ref) = refs
    dx = back_common(sizes, layer, (back_ref, dx_ref, dg_ref, router_ref, x_ref, x1_ref, c_ref, o_ref, qkv_ref, a_ref, dense_ref, col_ref, acc_ref, dqkv_ref, do_ref))
    dx_out[...] = dx
    combine_back(dx, router_low[...], col_ref[...], row_ref[...], layer - 1, picked_low, dg_out, send_ref)
    flush_dense(acc_ref, dense_out)


def last_kernel(sizes, *refs):
    (back_ref, dx_ref, dg_ref, router_ref, x_ref, x1_ref, c_ref, o_ref, qkv_ref, a_ref, dense_ref, col_ref, dx_out, dense_out, acc_ref, dqkv_ref, do_ref) = refs
    dx = back_common(sizes, 0, (back_ref, dx_ref, dg_ref, router_ref, x_ref, x1_ref, c_ref, o_ref, qkv_ref, a_ref, dense_ref, col_ref, acc_ref, dqkv_ref, do_ref))
    dx_out[...] = unpack_rows(dx, sizes[0], dx_out.shape[0] // sizes[0])
    flush_dense(acc_ref, dense_out)


class Shapes:
    def __init__(self, micros, images, rows, each, width, hidden, experts, slots_each, dense_rows, shards, groups):
        self.micros, self.images, self.rows, self.each = micros, images, rows, each
        self.width, self.hidden, self.experts, self.slots_each = width, hidden, experts, slots_each
        self.dense_rows, self.shards, self.groups = dense_rows, shards, groups
        self.toks = images * rows
        self.sizes = (images, rows, experts)

    def per_micro(self, *shape, dtype=F32):
        full = (self.micros, *shape)
        spec = pl.BlockSpec((None, *shape), lambda m: (m, *([0] * len(shape))))
        return spec, jax.ShapeDtypeStruct(full, dtype)

    def exchange(self):
        full = (self.experts, self.micros, self.slots_each, self.width)
        spec = pl.BlockSpec((self.experts, None, self.slots_each, self.width), lambda m: (0, m, 0, 0))
        return spec, jax.ShapeDtypeStruct(full, BF16)

    def token_block(self, dtype):
        per = self.images * self.each
        return pl.BlockSpec((per, self.width), lambda m: (m, 0)), jax.ShapeDtypeStruct((self.micros * per, self.width), dtype)

    def whole(self, *shape, dtype=BF16):
        spec = pl.BlockSpec(shape, lambda m: (0,) * len(shape), pipeline_mode=pl.Buffered(1))
        return spec, jax.ShapeDtypeStruct(shape, dtype)

    def forward_outs(self):
        t, w = self.toks, self.width
        return [
            self.per_micro(t, w),
            self.per_micro(t, 3 * w, dtype=BF16),
            self.per_micro(t, w, dtype=BF16),
            self.per_micro(t, w, dtype=BF16),
            self.per_micro(t, w),
            self.per_micro(t, w, dtype=BF16),
            self.per_micro(t, LANES),
            self.exchange(),
        ]

    def picked(self):
        return self.per_micro(2, self.toks, self.width, dtype=BF16)

    def cols(self):
        return self.per_micro(self.toks, LANES, dtype=jnp.int32)

    def row(self):
        return self.per_micro(8, self.toks, dtype=jnp.int32)

    def dense(self):
        return self.whole(self.dense_rows, self.width)

    def dense_out(self):
        return self.whole(self.shards, up_to(self.dense_rows // self.shards, 4 * self.groups), self.width)

    def scratch(self):
        return [
            pltpu.VMEM((self.dense_rows, self.width), F32),
            pltpu.VMEM((self.toks, 3 * self.width), BF16),
            pltpu.VMEM((self.toks, self.width), BF16),
        ]

    def saved_ins(self):
        t, w = self.toks, self.width
        return [self.exchange(), self.per_micro(t, w), self.per_micro(t, LANES), self.per_micro(t, LANES)] + self.forward_outs()[0:1] + [
            self.per_micro(t, w),
            self.per_micro(t, w, dtype=BF16),
            self.per_micro(t, w, dtype=BF16),
            self.per_micro(t, 3 * w, dtype=BF16),
            self.per_micro(t, w, dtype=BF16),
            self.dense(),
            self.cols(),
        ]

    def call(self, kernel, ins, outs, args, name, took, scratch=()):
        return pl.pallas_call(
            kernel,
            grid=(self.micros,),
            in_specs=[spec for spec, _ in ins],
            out_specs=[spec for spec, _ in outs],
            out_shape=[shape for _, shape in outs],
            scratch_shapes=list(scratch),
            compiler_params=pltpu.CompilerParams(vmem_limit_bytes=VMEM_LIMIT),
            cost_estimate=cost(took),
            name=name,
        )(*args)


def first_stage(shp, tokens, dense, cols, rows):
    return shp.call(
        functools.partial(first_kernel, shp.sizes),
        [shp.token_block(BF16), shp.dense(), shp.cols(), shp.row()],
        shp.forward_outs(),
        (tokens, dense, cols, rows),
        "attn_first",
        12,
    )


def middle_stage(shp, layer, back, x1, router, dense, cols, rows):
    t, w = shp.toks, shp.width
    return shp.call(
        functools.partial(middle_kernel, shp.sizes, layer),
        [shp.exchange(), shp.per_micro(t, w), shp.per_micro(t, LANES), shp.dense(), shp.cols(), shp.row()],
        [shp.picked(), *shp.forward_outs()],
        (back, x1, router, dense, cols, rows),
        "attn_next",
        16,
    )


def turn_stage(shp, layer, back, x1, router, cotangent, cols, rows):
    t, w = shp.toks, shp.width
    return shp.call(
        functools.partial(turn_kernel, shp.sizes, layer),
        [shp.exchange(), shp.per_micro(t, w), shp.per_micro(t, LANES), shp.token_block(BF16), shp.cols(), shp.row()],
        [shp.token_block(F32), shp.per_micro(t, w), shp.per_micro(t, LANES), shp.exchange()],
        (back, x1, router, cotangent, cols, rows),
        "turn",
        8,
        scratch=[pltpu.VMEM((2, t, w), BF16)],
    )


def back_stage(shp, layer, back, dx, dg, saved, dense, cols, rows, router_low, picked_low):
    t, w = shp.toks, shp.width
    x, qkv, a, o, x1, c, router = saved
    return shp.call(
        functools.partial(back_kernel, shp.sizes, layer),
        [*shp.saved_ins(), shp.row(), shp.per_micro(t, LANES), shp.picked()],
        [shp.per_micro(t, w), shp.per_micro(t, LANES), shp.exchange(), shp.dense_out()],
        (back, dx, dg, router, x, x1, c, o, qkv, a, dense, cols, rows, router_low, picked_low),
        "attn_back",
        28,
        scratch=shp.scratch(),
    )


def last_stage(shp, back, dx, dg, saved, dense, cols):
    x, qkv, a, o, x1, c, router = saved
    return shp.call(
        functools.partial(last_kernel, shp.sizes),
        shp.saved_ins(),
        [shp.token_block(F32), shp.dense_out()],
        (back, dx, dg, router, x, x1, c, o, qkv, a, dense, cols),
        "attn_last",
        25,
        scratch=shp.scratch(),
    )


def gelu_parts(h):
    cdf = 0.5 * (1.0 + lax.erf(h * INV_SQRT2))
    slope = cdf + h * (INV_SQRT2PI * jnp.exp(-0.5 * (h * h)))
    return (h * cdf).astype(BF16), slope.astype(BF16)


def adam_update(master, first_mom, second_mom, gradient, clip_scale, step_float):
    clipped = gradient * clip_scale
    first_new = BETA_ONE * first_mom + (1.0 - BETA_ONE) * clipped
    second_new = BETA_TWO * second_mom + (1.0 - BETA_TWO) * clipped * clipped
    first_hat = first_new / (1.0 - BETA_ONE**step_float)
    second_hat = second_new / (1.0 - BETA_TWO**step_float)
    change = -STEP_RATE * (first_hat / (jnp.sqrt(second_hat) + ADAM_EPS) + DECAY_RATE * master)
    return (change, first_new, second_new)


class Group:
    def __init__(self, cube, count):
        dp, ex = lax.axis_index("dp"), lax.axis_index("expert")
        self.cube, self.count, self.dp, self.ex = cube, count, dp, ex
        if cube:
            self.half, self.x, self.core = lax.div(ex, 4), lax.div(dp, 2), lax.rem(dp, 2)
            self.mine = lax.rem(self.half + self.x, 2) * 4 + lax.rem(ex, 4)
        else:
            self.mine = ex

    def device(self, expert):
        if self.cube:
            far = lax.rem(lax.div(expert, 4) + self.half, 2)
            return {"dp": far * 2 + self.core, "expert": self.half * 4 + lax.rem(expert, 4)}
        return {"dp": self.dp, "expert": expert}

    def after(self, steps):
        return lax.rem(self.mine + steps, self.count)

    def held_at(self, quarter):
        if self.cube:
            return lax.rem(quarter % 2 + self.core, 2) * 2 + lax.rem(quarter // 2 + self.x, 2)
        return quarter


def meet(devices):
    barrier = pltpu.get_barrier_semaphore()
    for device in devices:
        pl.semaphore_signal(barrier, inc=1, device_id=device, device_id_type=MESH)
    pl.semaphore_wait(barrier, len(devices))


def remote(src, dst, send_sem, recv_sem, device):
    return pltpu.make_async_remote_copy(
        src_ref=src, dst_ref=dst, send_sem=send_sem, recv_sem=recv_sem, device_id=device, device_id_type=MESH
    )


def dispatch_start(group, send, landed, ssem, rsem, lsem, micros):
    n = group.count
    for m in range(micros):
        pltpu.make_async_copy(send.at[group.mine, m], landed.at[m, 0], lsem.at[m]).start()
        for k in range(n - 1, 0, -1):
            target = group.after(k)
            remote(send.at[target, m], landed.at[m, n - k], ssem.at[m, k], rsem.at[m, n - k], group.device(target)).start()


def dispatch_wait(group, send, landed, ssem, rsem, m, slot):
    remote(send.at[0, 0], landed.at[m, slot], ssem.at[m, slot], rsem.at[m, slot], group.device(0)).wait_recv()


def return_start(group, ready, back, ysem, bsem, osem, m, slot):
    def away():
        remote(ready.at[m, slot], back.at[group.mine, m], ysem.at[m, slot], bsem.at[m, group.mine], group.device(group.after(slot))).start()

    if isinstance(slot, int):
        if slot == 0:
            pltpu.make_async_copy(ready.at[m, 0], back.at[group.mine, m], osem.at[m]).start()
        else:
            away()
        return

    @pl.when(slot == 0)
    def _():
        pltpu.make_async_copy(ready.at[m, 0], back.at[group.mine, m], osem.at[m]).start()

    @pl.when(slot > 0)
    def _():
        away()


def drain(group, send, landed, ready, back, ssem, rsem, ysem, bsem, osem, micros):
    n = group.count
    for m in range(micros):
        pltpu.make_async_copy(ready.at[m, 0], back.at[group.mine, m], osem.at[m]).wait()
        for k in range(1, n):
            there = group.device(0)
            remote(send.at[0, 0], landed.at[m, k], ssem.at[m, k], rsem.at[m, k], there).wait_send()
            remote(ready.at[m, k], back.at[0, m], ysem.at[m, k], bsem.at[m, 0], there).wait_send()
            who = group.after(k)
            remote(ready.at[m, k], back.at[who, m], ysem.at[m, k], bsem.at[m, who], there).wait_recv()


def load_weights(mats, wbuf, wsem):
    at = 0
    for i, ref in enumerate(mats):
        copy = pltpu.make_async_copy(ref, wbuf.at[pl.ds(at, ref.shape[0])], wsem.at[i])
        at += ref.shape[0]
        yield copy


def served_forward_kernel(cube, count, pieces, *refs):
    send, mats, (shift_ref, back, act_ref, slope_ref, keep_ref, landed, ready, wbuf, ssem, rsem, ysem, bsem, lsem, osem, wsem) = (
        refs[0],
        refs[1 : 1 + pieces],
        refs[1 + pieces :],
    )
    group = Group(cube, count)
    m, q = pl.program_id(0), pl.program_id(1)
    micros, chunks = landed.shape[0], count // (act_ref.shape[0] // landed.shape[2])
    each = count // chunks
    quarters, _, hidden = wbuf.shape
    width = landed.shape[3]
    part = 2 * width // quarters

    @pl.when((m == 0) & (q == 0))
    def _():
        for copy in load_weights(mats, wbuf, wsem):
            copy.start()
        meet([group.device(group.after(k)) for k in range(1, count)])
        dispatch_start(group, send, landed, ssem, rsem, lsem, micros)
        for copy in load_weights(mats, wbuf, wsem):
            copy.wait()

    for b in range(each):
        slot = q * each + b
        if b == 0:

            @pl.when(q == 0)
            def _():
                pltpu.make_async_copy(send.at[group.mine, m], landed.at[m, 0], lsem.at[m]).wait()

            @pl.when(q > 0)
            def _():
                dispatch_wait(group, send, landed, ssem, rsem, m, slot)
        else:
            dispatch_wait(group, send, landed, ssem, rsem, m, slot)
    x = landed[m, pl.ds(q * each, each)].reshape(act_ref.shape[0], width)
    keep_ref[...] = x
    if cube:
        span = (hidden + width) // quarters
        shift = jnp.concatenate(
            [wbuf[group.held_at(i), part:, :span].astype(F32)[0:1] for i in range(quarters)], axis=1
        )
    else:
        shift = shift_ref[...].astype(F32)
    y = [None] * (quarters // 2)
    for at in range(0, hidden, 512):
        cut = slice(at, at + 512)
        h = None
        for i in range(quarters // 2):
            piece = dot_nn(x[:, i * part : (i + 1) * part], wbuf[group.held_at(i), :part, cut])
            h = piece if h is None else h + piece
        act, slope = gelu_parts(h + shift[:, cut])
        act_ref[:, cut] = act
        slope_ref[:, cut] = slope
        for i in range(quarters // 2):
            piece = dot_nt(act, wbuf[group.held_at(quarters // 2 + i), :part, cut])
            y[i] = piece if y[i] is None else y[i] + piece
    y = (jnp.concatenate(y, axis=1) + shift[:, hidden:]).astype(BF16)
    ready[m, pl.ds(q * each, each)] = y.reshape(each, ready.shape[2], width)
    for b in range(each):
        if b == 0:
            return_start(group, ready, back, ysem, bsem, osem, m, q * each)
        else:
            slot = q * each + b
            remote(ready.at[m, slot], back.at[group.mine, m], ysem.at[m, slot], bsem.at[m, group.mine], group.device(group.after(slot))).start()

    @pl.when((m == micros - 1) & (q == chunks - 1))
    def _():
        drain(group, send, landed, ready, back, ssem, rsem, ysem, bsem, osem, micros)


def any_spec():
    return pl.BlockSpec(memory_space=pl.ANY)


def comm_params(ident):
    return pltpu.CompilerParams(vmem_limit_bytes=VMEM_LIMIT, collective_id=ident, has_side_effects=True)


def exchange_sems(micros, count):
    table = pltpu.SemaphoreType.DMA((micros, count))
    return [table] * 4 + [pltpu.SemaphoreType.DMA((micros,))] * 2 + [pltpu.SemaphoreType.DMA((2,))]


def served_forward(cube, send, mats, shift):
    count, micros, slots, width = send.shape
    chunks = 4
    rows = count // chunks * slots
    quarters = sum(x.shape[0] for x in mats)
    block, hidden = mats[0].shape[1:]
    row_spec = lambda cols: pl.BlockSpec((None, rows, cols), lambda m, q: (m, q, 0))
    full = (micros, count * slots)
    return pl.pallas_call(
        functools.partial(served_forward_kernel, cube, count, len(mats)),
        grid=(micros, chunks),
        in_specs=[any_spec()] * (1 + len(mats)) + [pl.BlockSpec(shift.shape, lambda m, q: (0, 0))],
        out_specs=[any_spec(), row_spec(hidden), row_spec(hidden), row_spec(width)],
        out_shape=[
            jax.ShapeDtypeStruct(send.shape, BF16),
            jax.ShapeDtypeStruct((*full, hidden), BF16),
            jax.ShapeDtypeStruct((*full, hidden), BF16),
            jax.ShapeDtypeStruct((*full, width), BF16),
        ],
        scratch_shapes=[
            pltpu.VMEM((micros, count, slots, width), BF16),
            pltpu.VMEM((micros, count, slots, width), BF16),
            pltpu.VMEM((quarters, block, hidden), BF16),
            *exchange_sems(micros, count),
        ],
        compiler_params=comm_params(0),
        cost_estimate=cost(48),
        name="served_forward",
    )(send, *mats, shift)


def served_back_kernel(cube, count, pieces, *refs):
    send, mats, refs = refs[0], refs[1 : 1 + pieces], refs[1 + pieces :]
    (x_ref, act_ref, slope_ref, back, *dw_refs, landed, ready, wbuf, xt_ref, dyt_ref, total_ref, acc_ref, bias_ref, ssem, rsem, ysem, bsem, lsem, osem, wsem) = refs
    group = Group(cube, count)
    m, f = pl.program_id(0), pl.program_id(1)
    micros, steps = pl.num_programs(0), pl.num_programs(1)
    total_micros = landed.shape[0]
    quarters, block, _ = wbuf.shape
    slots, width = landed.shape[2:]
    rows = count * slots
    part = 2 * width // quarters
    wide = act_ref.shape[1]
    cut = pl.ds(pl.multiple_of(f * wide, wide), wide)

    @pl.when((m == 0) & (f == 0))
    def _():
        for copy in load_weights(mats, wbuf, wsem):
            copy.start()
        meet([group.device(group.after(k)) for k in range(1, count)])
        dispatch_start(group, send, landed, ssem, rsem, lsem, total_micros)
        for copy in load_weights(mats, wbuf, wsem):
            copy.wait()

    @pl.when(f == 0)
    def _():
        xt_ref[...] = x_ref[...].T
        pltpu.make_async_copy(send.at[group.mine, m], landed.at[m, 0], lsem.at[m]).wait()
        for slot in range(1, count):
            dispatch_wait(group, send, landed, ssem, rsem, m, slot)
        dyt_ref[...] = landed[m].reshape(rows, width).T
        total_ref[...] = jnp.zeros_like(total_ref)

    dy = landed[m].reshape(rows, width)
    dact = None
    for i in range(quarters // 2):
        piece = dot_nn(dy[:, i * part : (i + 1) * part], wbuf[group.held_at(quarters // 2 + i), :part, cut])
        dact = piece if dact is None else dact + piece
    dh = (dact * slope_ref[...].astype(F32)).astype(BF16)
    act = act_ref[...]
    first = m == 0
    spans = width // wide
    dy_cut = landed[m, :, :, pl.ds(pl.multiple_of(lax.rem(f, spans) * wide, wide), wide)].reshape(rows, wide)
    dy_sum = jnp.where(f < spans, jnp.sum(dy_cut.astype(F32), axis=0, keepdims=True), 0.0)
    bias = jnp.concatenate(
        [jnp.sum(dh.astype(F32), axis=0, keepdims=True), dy_sum, jnp.zeros((block - part - 2, wide), F32)], axis=0
    ) + jnp.where(first, 0.0, bias_ref[f])
    bias_ref[f] = bias
    for i in range(quarters):
        left = xt_ref if i < quarters // 2 else dyt_ref
        at = (i % (quarters // 2)) * part
        grad = dot_nn(left[at : at + part, :], dh if i < quarters // 2 else act)
        grad = grad + jnp.where(first, 0.0, acc_ref[f, i])
        acc_ref[f, i] = grad
        low = jnp.concatenate([grad, bias], axis=0).astype(BF16)
        if cube:

            @pl.when(group.core == i % 2)
            def _():
                dw_refs[0][i // 2] = low

            @pl.when(group.core != i % 2)
            def _():
                dw_refs[1][i // 2] = low
        else:
            dw_refs[0][i] = low
    for i in range(quarters // 2):
        total_ref[:, i * part : (i + 1) * part] += dot_nt(dh, wbuf[group.held_at(i), :part, cut])

    @pl.when(f == steps - 1)
    def _():
        ready[m] = total_ref[...].astype(BF16).reshape(count, slots, width)
        for slot in range(count):
            return_start(group, ready, back, ysem, bsem, osem, m, slot)

    @pl.when((m == micros - 1) & (f == steps - 1))
    def _():
        drain(group, send, landed, ready, back, ssem, rsem, ysem, bsem, osem, total_micros)


def served_back(cube, send, mats, x, act, slope):
    count, micros, slots, width = send.shape
    rows = count * slots
    quarters = sum(v.shape[0] for v in mats)
    block, hidden = mats[0].shape[1:]
    part = 2 * width // quarters
    wide = 256
    steps = hidden // wide
    outs = 2 if cube else 1
    col_spec = pl.BlockSpec((None, rows, wide), lambda m, f: (m, 0, f))
    return pl.pallas_call(
        functools.partial(served_back_kernel, cube, count, len(mats)),
        grid=(micros, steps),
        in_specs=[any_spec()] * (1 + len(mats)) + [pl.BlockSpec((None, rows, width), lambda m, f: (m, 0, 0)), col_spec, col_spec],
        out_specs=[any_spec()] + [pl.BlockSpec((quarters // outs, block, wide), lambda m, f: (0, 0, lax.div(m, micros - 1) * f if micros > 1 else f))] * outs,
        out_shape=[jax.ShapeDtypeStruct(send.shape, BF16)] + [jax.ShapeDtypeStruct((quarters // outs, block, hidden), BF16)] * outs,
        scratch_shapes=[
            pltpu.VMEM((micros, count, slots, width), BF16),
            pltpu.VMEM((micros, count, slots, width), BF16),
            pltpu.VMEM((quarters, block, hidden), BF16),
            pltpu.VMEM((width, rows), BF16),
            pltpu.VMEM((width, rows), BF16),
            pltpu.VMEM((rows, width), F32),
            pltpu.VMEM((steps, quarters, part, wide), F32),
            pltpu.VMEM((steps, block - part, wide), F32),
            *exchange_sems(micros, count),
        ],
        compiler_params=comm_params(1),
        cost_estimate=cost(60),
        name="served_back",
    )(send, *mats, x, act, slope)


def dense_sum_kernel(shards, groups, g_ref, out_ref, landed, part_ref, total_ref, spread, s1, r1, s2, r2, s3, r3):
    dp, ex = lax.axis_index("dp"), lax.axis_index("expert")
    rows = part_ref.shape[0]
    each = rows * 4 // groups
    line = [{"dp": dp, "expert": lax.rem(ex + k, groups)} for k in range(1, groups)]
    if shards == 4:
        x, core = lax.div(dp, 2), lax.rem(dp, 2)
        near, far = {"dp": x * 2 + 1 - core, "expert": ex}, {"dp": (1 - x) * 2 + core, "expert": ex}
        meet([near, far] + line)
        copies = []
        for k in range(2):
            copy = remote(g_ref.at[k * 2 + 1 - core], landed.at[k], s1.at[k], r1.at[k], near)
            copy.start()
            copies.append(copy)
        for copy in copies:
            copy.wait()
        landed[3] = (g_ref[(1 - x) * 2 + core].astype(F32) + landed[1 - x].astype(F32)).astype(BF16)
        copy = remote(landed.at[3], landed.at[2], s1.at[2], r1.at[2], far)
        copy.start()
        total = g_ref[x * 2 + core].astype(F32) + landed[x].astype(F32)
        copy.wait()
        part_ref[...] = (total + landed[2].astype(F32)).astype(BF16)
    else:
        column = [{"dp": lax.rem(dp + k, shards), "expert": ex} for k in range(1, shards)]
        meet(column + line)
        copies = []
        for k in range(1, shards):
            copy = remote(g_ref.at[lax.rem(dp + k, shards)], landed.at[shards - k], s1.at[k], r1.at[shards - k], column[k - 1])
            copy.start()
            copies.append(copy)
        for copy in copies:
            copy.wait()
        total = g_ref[dp].astype(F32)
        for k in range(1, shards):
            total = total + landed[k].astype(F32)
        part_ref[...] = total.astype(BF16)

    def piece(ref, j):
        if groups >= 4:
            span = groups // 4
            return ref.at[pl.ds(pl.multiple_of(lax.rem(j, span) * each, 16), each), pl.ds(pl.multiple_of(lax.div(j, span) * LANES, LANES), LANES)]
        raise ValueError("groups")

    copies = []
    for k in range(1, groups):
        copy = remote(piece(part_ref, lax.rem(ex + k, groups)), spread.at[groups - k], s2.at[k], r2.at[groups - k], line[k - 1])
        copy.start()
        copies.append(copy)
    span = groups // 4
    mine_rows = pl.ds(pl.multiple_of(lax.rem(ex, span) * each, 16), each)
    mine_cols = pl.ds(pl.multiple_of(lax.div(ex, span) * LANES, LANES), LANES)
    mine = part_ref[mine_rows, mine_cols].astype(F32)
    for copy in copies:
        copy.wait()
    for k in range(1, groups):
        mine = mine + spread[k].astype(F32)
    total_ref[...] = mine.astype(BF16)
    copies = []
    for k in range(1, groups):
        copy = remote(total_ref, piece(out_ref, ex), s3.at[k], r3.at[groups - k], line[k - 1])
        copy.start()
        copies.append(copy)
    out_ref[mine_rows, mine_cols] = total_ref[...]
    for copy in copies:
        copy.wait()


def dense_sum(grad, groups):
    shards, rows, width = grad.shape
    each = rows * 4 // groups
    vmem = pl.BlockSpec(memory_space=pltpu.VMEM)
    return pl.pallas_call(
        functools.partial(dense_sum_kernel, shards, groups),
        in_specs=[vmem],
        out_specs=vmem,
        out_shape=jax.ShapeDtypeStruct((rows, width), BF16),
        scratch_shapes=[
            pltpu.VMEM((shards, rows, width), BF16),
            pltpu.VMEM((rows, width), BF16),
            pltpu.VMEM((each, LANES), BF16),
            pltpu.VMEM((groups, each, LANES), BF16),
            pltpu.SemaphoreType.DMA((shards,)),
            pltpu.SemaphoreType.DMA((shards,)),
            pltpu.SemaphoreType.DMA((groups,)),
            pltpu.SemaphoreType.DMA((groups,)),
            pltpu.SemaphoreType.DMA((groups,)),
            pltpu.SemaphoreType.DMA((groups,)),
        ],
        compiler_params=comm_params(2),
        cost_estimate=cost(50),
        name="dense_sum",
    )(grad)


def scalar_sum_kernel(shards, groups, x_ref, out_ref, near, line_total, far, s1, r1, s2, r2):
    dp, ex = lax.axis_index("dp"), lax.axis_index("expert")
    column = [{"dp": lax.rem(dp + k, shards), "expert": ex} for k in range(1, shards)]
    line = [{"dp": dp, "expert": lax.rem(ex + k, groups)} for k in range(1, groups)]
    meet(column + line)
    copies = []
    for k in range(1, groups):
        copy = remote(x_ref, near.at[ex], s1.at[k], r1.at[ex], line[k - 1])
        copy.start()
        copies.append(copy)
    near[ex] = x_ref[...]
    for k in range(1, groups):
        copies[k - 1].wait_send()
        who = lax.rem(ex + k, groups)
        remote(x_ref, near.at[who], s1.at[k], r1.at[who], line[k - 1]).wait_recv()
    total = near[0]
    for j in range(1, groups):
        total = total + near[j]
    line_total[...] = total
    copies = []
    for k in range(1, shards):
        copy = remote(line_total, far.at[dp], s2.at[k], r2.at[dp], column[k - 1])
        copy.start()
        copies.append(copy)
    far[dp] = total
    for k in range(1, shards):
        copies[k - 1].wait_send()
        who = lax.rem(dp + k, shards)
        remote(line_total, far.at[who], s2.at[k], r2.at[who], column[k - 1]).wait_recv()
    total = far[0]
    for j in range(1, shards):
        total = total + far[j]
    out_ref[...] = jnp.broadcast_to(jnp.sum(total, keepdims=True), total.shape)


def scalar_sum(value, shards, groups):
    tile = (8, LANES)
    vmem = pl.BlockSpec(memory_space=pltpu.VMEM)
    return pl.pallas_call(
        functools.partial(scalar_sum_kernel, shards, groups),
        in_specs=[vmem],
        out_specs=vmem,
        out_shape=jax.ShapeDtypeStruct(tile, F32),
        scratch_shapes=[
            pltpu.VMEM((groups, *tile), F32),
            pltpu.VMEM(tile, F32),
            pltpu.VMEM((shards, *tile), F32),
            pltpu.SemaphoreType.DMA((groups,)),
            pltpu.SemaphoreType.DMA((groups,)),
            pltpu.SemaphoreType.DMA((shards,)),
            pltpu.SemaphoreType.DMA((shards,)),
        ],
        compiler_params=comm_params(3),
        cost_estimate=cost(10),
        name="scalar_sum",
    )(value)[0, 0]


def shifted(values, move):
    shards, groups = lax.axis_size("dp"), lax.axis_size("expert")
    pairs = []
    for d in range(shards):
        for e in range(groups):
            to = {"z": (d, (e + 4) % 8), "x": ((d + 2) % 4, e), "core": (d ^ 1, e)}[move]
            pairs.append((d * groups + e, to[0] * groups + to[1]))
    return lax.ppermute(values, ("dp", "expert"), pairs)


def on_first_x():
    return lax.div(lax.axis_index("dp"), 2) == 0


def x_turn(rows, partner):
    return jnp.where(on_first_x(), partner, rows)


def pair_up(rows, partner, far):
    return jnp.stack([jnp.where(on_first_x(), rows, partner), far])


def together(*values):
    return lax.optimization_barrier(values)


def dense_gather_kernel(low_ref, *refs):
    outs, (landed, wide_ref, own_sem, send_sem, recv_sem) = refs[: low_ref.shape[0]], refs[low_ref.shape[0] :]
    dp, ex = lax.axis_index("dp"), lax.axis_index("expert")
    x, core = lax.div(dp, 2), lax.rem(dp, 2)
    near, far = {"dp": x * 2 + 1 - core, "expert": ex}, {"dp": (1 - x) * 2 + core, "expert": ex}
    layers, rows, _ = low_ref.shape
    meet([near, far])
    own, across, beside, passed = [], [], [], []
    for i in range(layers):
        across.append(remote(low_ref.at[i], landed.at[i, 1], send_sem.at[i, 1], recv_sem.at[i, 1], far))
        across[i].start()
        beside.append(remote(low_ref.at[i], landed.at[i, 2], send_sem.at[i, 2], recv_sem.at[i, 2], near))
        beside[i].start()
        own.append(pltpu.make_async_copy(low_ref.at[i], landed.at[i, 0], own_sem.at[i]))
        own[i].start()
    for i in range(layers):
        across[i].wait()
        passed.append(remote(landed.at[i, 1], landed.at[i, 3], send_sem.at[i, 3], recv_sem.at[i, 3], near))
        passed[i].start()
        own[i].wait()
        beside[i].wait()
        passed[i].wait()
        for s in range(4):
            spot = lax.rem(s // 2 + x, 2) + 2 * lax.rem(s % 2 + core, 2)
            wide_ref[s * rows : (s + 1) * rows, :] = landed[i, spot].astype(F32)
        outs[i][...] = wide_ref[...].astype(BF16)


def dense_gather(low):
    layers, rows, width = low.shape
    vmem = pl.BlockSpec(memory_space=pltpu.VMEM)
    return pl.pallas_call(
        dense_gather_kernel,
        in_specs=[vmem],
        out_specs=[vmem] * layers,
        out_shape=[jax.ShapeDtypeStruct((4 * rows, width), BF16)] * layers,
        scratch_shapes=[
            pltpu.VMEM((layers, 4, rows, width), BF16),
            pltpu.VMEM((4 * rows, width), F32),
            pltpu.SemaphoreType.DMA((layers,)),
            pltpu.SemaphoreType.DMA((layers, 4)),
            pltpu.SemaphoreType.DMA((layers, 4)),
        ],
        compiler_params=comm_params(4),
        cost_estimate=cost(30),
        name="dense_gather",
    )(low)


def pack_kernel(master_ref, shift_ref, out_ref):
    part, hidden = master_ref.shape
    rows = out_ref.shape[0] - part
    span = shift_ref.shape[1]
    out_ref[:part, :] = master_ref[...].astype(BF16)
    wide = jnp.concatenate([shift_ref[...], jnp.zeros((1, hidden - span), F32)], axis=1)
    subs = lax.broadcasted_iota(jnp.int32, (rows, hidden), 0)
    out_ref[part:, :] = jnp.where(subs == 0, wide, 0.0).astype(BF16)


def pack(master, shift, layer, rows):
    part, hidden = master.shape[2:]
    span = shift.shape[2]
    return pl.pallas_call(
        pack_kernel,
        grid=(1,),
        in_specs=[
            pl.BlockSpec((None, None, part, hidden), lambda g: (layer, 0, 0, 0)),
            pl.BlockSpec((None, 1, span), lambda g: (layer, 0, 0)),
        ],
        out_specs=pl.BlockSpec((rows, hidden), lambda g: (0, 0)),
        out_shape=jax.ShapeDtypeStruct((rows, hidden), BF16),
        compiler_params=pltpu.CompilerParams(vmem_limit_bytes=VMEM_LIMIT),
        cost_estimate=cost(3),
        name="pack",
    )(master, shift)


def tile_square(values):
    rows, cols = values.shape
    folded = jnp.sum((values * values).reshape(rows // 8, 8, cols), axis=0)
    total = folded[:, :LANES]
    for at in range(LANES, cols, LANES):
        total = total + folded[:, at : at + LANES]
    return total


def finish_kernel(layers, width, *refs):
    nears, lasts, sums = refs[:layers], refs[layers : 2 * layers], refs[2 * layers : 3 * layers]
    grad_ref, shift_ref, square_ref = refs[3 * layers :]
    dp, ex = lax.axis_index("dp"), lax.axis_index("expert")
    part = grad_ref.shape[2]
    span = shift_ref.shape[2]
    total = jnp.zeros((8, LANES), F32)
    subs = lax.broadcasted_iota(jnp.int32, (8, span), 0)
    for i in range(layers):
        grad = nears[i][...] + lasts[i][...].astype(F32)
        grad_ref[i, 0] = grad[:part]
        total = total + tile_square(grad[:part])
        full = jnp.concatenate([grad[part : part + 1], grad[part + 1 : part + 2, :width]], axis=1)
        mine = jnp.zeros((1, span), F32)
        for q in range(full.shape[1] // span):
            mine = jnp.where(dp == q, full[:, q * span : (q + 1) * span], mine)
        shift_ref[i] = mine
        total = total + tile_square(jnp.where(subs == 0, mine, 0.0))
        dense = sums[i][...].astype(F32)
        total = total + jnp.where(ex == 0, tile_square(dense), 0.0)
    square_ref[...] = total


def finish(pieces, sums, shards, part, span, width):
    layers = len(pieces)
    hidden = pieces[0][0].shape[1]
    vmem = pl.BlockSpec(memory_space=pltpu.VMEM)
    return pl.pallas_call(
        functools.partial(finish_kernel, layers, width),
        in_specs=[vmem] * (3 * layers),
        out_specs=[vmem] * 3,
        out_shape=[
            jax.ShapeDtypeStruct((layers, 1, part, hidden), F32),
            jax.ShapeDtypeStruct((layers, 1, span), F32),
            jax.ShapeDtypeStruct((8, LANES), F32),
        ],
        compiler_params=pltpu.CompilerParams(vmem_limit_bytes=VMEM_LIMIT),
        cost_estimate=cost(5),
        name="finish",
    )(*[near for near, _ in pieces], *[last for _, last in pieces], *sums)


def served_shift(served, part, span):
    return jnp.concatenate([v[:, part, :span] for v in served]).reshape(1, -1)


def local(
    tokens,
    cotangent,
    valid,
    routes,
    priority,
    step,
    dense_master,
    dense_first,
    dense_second,
    expert_master,
    expert_first,
    expert_second,
    shift_master,
    shift_first,
    shift_second,
):
    layer_count, shard_rows, width = dense_master.shape
    micros, group_tok = priority.shape
    each = valid.shape[1]
    images = group_tok // each
    hidden = expert_master.shape[3]
    groups = lax.axis_size("expert")
    shards = lax.axis_size("dp")
    experts = expert_master.shape[1] * groups
    capacity = (9 * images * PATCHES + 4 * experts - 1) // (4 * experts)
    slots_each = up_to(capacity, 16)
    rows = up_to(PATCHES, 16)
    shp = Shapes(micros, images, rows, each, width, hidden, experts, slots_each, shard_rows * shards, shards, groups)

    cube = shards == 4 and groups == 8
    part, span = expert_master.shape[2], shift_master.shape[2]
    row_block = up_to(part + 2, 16)

    def owned_rows(i):
        extra = jnp.pad(shift_master[i], ((0, row_block - part - 1), (0, hidden - span)))
        return jnp.concatenate([expert_master[i, 0], extra], axis=0).astype(BF16)

    own = [pack(expert_master, shift_master, i, row_block) if cube else owned_rows(i) for i in range(layer_count)]
    dense_low = jnp.stack([dense_master[i].astype(BF16) for i in range(layer_count)])
    slot_col, slot_row = routing(
        priority, valid, jnp.swapaxes(routes, 1, 2), capacity, slots_each, experts, rows
    )
    if cube:
        partner = shifted(own[0], "z")
        dense = dense_gather(dense_low)
        tokens, slot_col, crossing = together(tokens, slot_col, x_turn(own[0], partner))
        far = shifted(crossing, "x")
        later, _ = together(own[1], crossing)
        partners = [partner, shifted(later, "z")]
    else:
        dense = [lax.all_gather(dense_low[i], "dp", axis=0, tiled=True) for i in range(layer_count)]
        mats = [(lax.all_gather(own[i], "dp", axis=0),) for i in range(layer_count)]

    saved, kept, picks, mats_in = [], [], [], []
    for i in range(layer_count):
        if i == 0:
            outs = first_stage(shp, tokens, dense[0], slot_col, slot_row)
        else:
            picked, *outs = middle_stage(shp, i, back, saved[i - 1][4], saved[i - 1][6], dense[i], slot_col, slot_row)
            picks.append(picked)
        *state, send = outs
        saved.append(state)
        if cube:
            if i:
                pair = pair_up(own[i], partners[i], far)
            else:
                pair = pair_up(own[0], partner, far)
            pair, send = together(pair, send)
            served = (pair, shifted(pair, "core"))
            mats_in.append(served)
        else:
            mats_in.append(mats[i])
        shift = jnp.zeros((8, LANES), BF16) if cube else served_shift(mats_in[i], part, span)
        back, act, slope, received = served_forward(cube, send, mats_in[i], shift)
        if cube and i + 1 < layer_count:
            partners[i + 1], back = together(partners[i + 1], back)
            crossing = x_turn(own[i + 1], partners[i + 1])
            far = shifted(crossing, "x")
        kept.append((received, act, slope))
    top = layer_count - 1
    output, dx, dg, send = turn_stage(shp, top, back, saved[top][4], saved[top][6], cotangent, slot_col, slot_row)
    dense_grads, mats_grads = [None] * layer_count, [None] * layer_count
    for i in reversed(range(layer_count)):
        received, act, slope = kept[i]
        back, grads, *others = served_back(cube, send, mats_in[i], received, act, slope)
        if not cube:
            mats_grads[i] = lax.psum_scatter(grads, "dp", scatter_dimension=0, tiled=False)
        beside = shifted(others[0], "core") if cube else None
        if i:
            dx, dg, send, dense_grads[i] = back_stage(
                shp, i, back, dx, dg, saved[i], dense[i], slot_col, slot_row, saved[i - 1][6], picks[i - 1]
            )
            if cube:
                near_pair = grads.astype(F32) + beside.astype(F32)
                crossing, send = together(jnp.where(on_first_x(), near_pair[1], near_pair[0]).astype(BF16), send)
                far = shifted(crossing, "x")
                waiting = (near_pair, far)
        else:
            if cube:
                upper_pair, upper_far = waiting
                onward = jnp.where(on_first_x(), upper_far, upper_pair[1].astype(BF16))
                near_pair = grads.astype(F32) + beside.astype(F32)
                crossing = jnp.where(on_first_x(), near_pair[1], near_pair[0]).astype(BF16)
                onward, crossing, back = together(onward, crossing, back)
                upper_last = shifted(onward, "z")
                mats_grads[1] = (jnp.where(on_first_x(), upper_pair[0], upper_far.astype(F32)), upper_last)
                far = shifted(crossing, "x")
            grad_tokens, dense_grads[i] = last_stage(shp, back, dx, dg, saved[i], dense[i], slot_col)
            if cube:
                onward, dense_grads[i] = together(jnp.where(on_first_x(), far, near_pair[1].astype(BF16)), dense_grads[i])
                mats_grads[0] = (jnp.where(on_first_x(), near_pair[0], far.astype(F32)), shifted(onward, "z"))
    dense_sums = []
    for i in range(layer_count):
        if i:
            dense_sums.append(lax.psum(lax.psum_scatter(dense_grads[i], "dp", scatter_dimension=0, tiled=False), "expert"))
        else:
            dense_sums.append(dense_sum(dense_grads[i], groups))
    fold = lambda v: v.reshape(layer_count, shard_rows, width // LANES, LANES).transpose(1, 2, 0, 3).reshape(-1, LANES)
    unfold = lambda v: v.reshape(shard_rows, width // LANES, layer_count, LANES).transpose(2, 0, 1, 3).reshape(layer_count, shard_rows, width)
    dense_shard = fold(jnp.stack([g[:shard_rows] for g in dense_sums]).astype(F32))
    if cube:
        expert_shard, shift_shard, square = finish(mats_grads, dense_sums, shards, part, span, width)
    else:
        owned = [g.astype(F32) for g in mats_grads]
        expert_shard = jnp.stack([g[:part] for g in owned])[:, None]
        shift_shard = jnp.stack(
            [lax.dynamic_slice(jnp.concatenate([g[part], g[part + 1, :width]]), (lax.axis_index("dp") * span,), (span,)) for g in owned]
        )[:, None]
        first_replica = (lax.axis_index("expert") == 0).astype(F32)
        square = (
            jnp.sum(dense_shard * dense_shard) * first_replica
            + jnp.sum(expert_shard * expert_shard)
            + jnp.sum(shift_shard * shift_shard)
        )
        square = jnp.zeros((8, LANES), F32).at[0, 0].set(square)
    grad_norm = jnp.sqrt(scalar_sum(square, shards, groups))
    clip_scale = CLIP_NORM / jnp.maximum(grad_norm, CLIP_NORM)
    step_float = step.astype(F32)
    dense_new = adam_update(fold(dense_master), fold(dense_first), fold(dense_second), dense_shard, clip_scale, step_float)
    dense_new = [unfold(values) for values in dense_new]
    expert_new = adam_update(expert_master, expert_first, expert_second, expert_shard, clip_scale, step_float)
    shift_new = adam_update(shift_master, shift_first, shift_second, shift_shard, clip_scale, step_float)
    return (output, grad_tokens, grad_norm, unfold(dense_shard), *dense_new, expert_shard, *expert_new, shift_shard, *shift_new)


def solution(mesh):
    split = P(("dp", "expert"), None)
    dense = P(None, "dp", None)
    mats = P(None, "expert", "dp", None)
    shift = P(None, "expert", "dp")
    placed = (split, split, split, P(None, ("dp", "expert"), None), split, P()) + (dense,) * 3 + (mats,) * 3 + (shift,) * 3
    return jax.shard_map(
        local,
        mesh=mesh,
        in_specs=placed,
        out_specs=(split, split, P()) + (dense,) * 4 + (mats,) * 4 + (shift,) * 4,
        check_vma=False,
    )
```
